32 devices in a mesh: seq: 8 (over z, y), ch: 4 (over x, core).
Axes of the slice: x: 2, y: 2, z: 4, core: 2. Of those that a mesh axis runs over, the one named last changes fastest.
Arguments:
- query_proj: float32 [64, 8192], P('ch', 'seq'), may hold values from -6 to 6
- key_proj: float32 [64, 8192], P('ch', 'seq'), may hold values from -6 to 6
- value_proj: float32 [64, 8192], P('ch', 'seq'), may hold values from -6 to 6
- filter_taps: float32 [64, 8192], P('ch', 'seq'), may hold values from -6 to 6
- out_cotangent: float32 [64, 8192], P('ch', 'seq'), may hold values from -6 to 6
Outputs:
- hyena_out: float32 [64, 8192], P('ch', 'seq')
- query_grad: float32 [64, 8192], P('ch', 'seq')
- key_grad: float32 [64, 8192], P('ch', 'seq')
- value_grad: float32 [64, 8192], P('ch', 'seq')
- filter_grad: float32 [64, 8192], P('ch', 'seq')
The draws below stay inside these ranges and needn't reach their ends.
All inputs are finite; a program needn't handle non-finite values.
Results may differ from the reference program's by a relative error of at most 0.000098.
Values sent between devices are 32-bit elements; how exact they have to be, the bound alone decides.
No kernel may reach another device: no remote copies, remote signals or barrier semaphores. Data moves between devices by JAX's collectives and lax.ppermute only.
A program may use at most 64 MiB of HBM per device.

```python
import jax
import jax.numpy as jnp

SEQ = 8192
CH = 64


def steps_of(key, shape, shards, low, high):
    gain = 1.0
    for axis_at, shards_of in shards:
        steps = jax.random.uniform(jax.random.fold_in(jax.random.fold_in(key, 6), axis_at), (shards_of,), jnp.float32, low / len(shards), high / len(shards))
        gain = gain * jnp.repeat(jnp.exp(steps), shape[axis_at] // shards_of).reshape((-1,) + (1,) * (len(shape) - 1 - axis_at))
    return gain


def bell_draw(rng, dims, deviation, limit, split=(), held_as=jnp.bfloat16):
    array = deviation * jax.random.normal(rng, dims, jnp.float32)
    if split:
        array = array * steps_of(rng, dims, split, -0.22, 0.18)
    return jnp.clip(array, -limit, limit).astype(held_as)


def setup_inputs(seed: int = 0) -> dict:
    streams_of = jax.random.split(jax.random.key(seed), 6)
    return {
        "query_proj": bell_draw(streams_of[0], (CH, SEQ), 1.0, 6.0, ((0, 4), (1, 8)), jnp.float32),
        "key_proj": bell_draw(streams_of[1], (CH, SEQ), 1.0, 6.0, ((0, 4), (1, 8)), jnp.float32),
        "value_proj": bell_draw(streams_of[2], (CH, SEQ), 1.0, 6.0, ((0, 4), (1, 8)), jnp.float32),
        "filter_taps": bell_draw(streams_of[3], (CH, SEQ), 1.0, 6.0, ((0, 4), (1, 8)), jnp.float32),
        "out_cotangent": bell_draw(streams_of[4], (CH, SEQ), 1.0, 6.0, ((0, 4), (1, 8)), jnp.float32),
    }


def reference(query_proj, key_proj, value_proj, filter_taps, out_cotangent):
    full_len = 2 * SEQ
    factor = SEQ ** -0.5
    gated = key_proj * value_proj
    weighted = out_cotangent * query_proj
    gated_spec = jnp.fft.rfft(gated, n=full_len, axis=1)
    filter_spec = jnp.fft.rfft(filter_taps, n=full_len, axis=1)
    weighted_spec = jnp.fft.rfft(weighted, n=full_len, axis=1)
    mixed = jnp.fft.irfft(filter_spec * gated_spec, n=full_len, axis=1)[:, :SEQ] * factor
    gated_grad = jnp.fft.irfft(jnp.conj(filter_spec) * weighted_spec, n=full_len, axis=1)[:, :SEQ] * factor
    filter_grad = jnp.fft.irfft(jnp.conj(gated_spec) * weighted_spec, n=full_len, axis=1)[:, :SEQ] * factor
    mixed = mixed.astype(query_proj.dtype)
    gated_grad = gated_grad.astype(query_proj.dtype)
    filter_grad = filter_grad.astype(query_proj.dtype)
    return (query_proj * mixed, out_cotangent * mixed, gated_grad * value_proj, gated_grad * key_proj, filter_grad)
```

```python
import math

import jax
import jax.numpy as jnp
import numpy as np
from jax import lax
from jax.experimental import pallas as pl
from jax.experimental.pallas import tpu as pltpu
from jax.sharding import PartitionSpec as P

FAC = 512
LANES = 128
SUBLANES = 8


exact_mode = lax.Precision.HIGHEST


def angle_grid(row_ids, col_ids, period):
    angles = (row_ids * col_ids % period).astype(jnp.float32) * (2.0 * math.pi / period)
    return (jnp.cos(angles), jnp.sin(angles))


def index_grid(row_count, col_count):
    return (
        lax.broadcasted_iota(jnp.int32, (row_count, col_count), 0),
        lax.broadcasted_iota(jnp.int32, (row_count, col_count), 1),
    )


def grad_items(first_grad, second_grad):
    return ([first_grad, second_grad], False)


def bins_over_devices(query_proj, key_proj, value_proj, filter_taps, out_cotangent):
    devices = lax.axis_size("seq")
    position = lax.axis_index("seq")
    channels = filter_taps.shape[0]
    tokens = filter_taps.shape[1]
    run_count = tokens // FAC
    half_first = run_count * devices
    first_len = 2 * half_first
    col_group = FAC // devices
    full_len = first_len * FAC
    width_cg = channels * col_group
    out_scale = 1.0 / (full_len * math.sqrt(tokens * devices))
    slot_count = first_len // devices
    time_ids, bin_ids = index_grid(half_first, first_len)
    cos_first, sin_first = angle_grid(time_ids, bin_ids, first_len)
    fwd_imag = -sin_first
    inv_imag = -sin_first
    bin_rows, lane_ids = index_grid(first_len, width_cg)
    cos_turn, sin_turn = angle_grid(bin_rows, position * col_group + lane_ids % col_group, full_len)
    square_rows, square_cols = index_grid(FAC, FAC)
    cos_second, sin_second = angle_grid(square_rows, square_cols, FAC)
    cos_grid = cos_second.reshape(devices, col_group, FAC)
    sin_grid = sin_second.reshape(devices, col_group, FAC)
    cos_back = cos_second.reshape(FAC, devices, col_group)
    sin_back = sin_second.reshape(FAC, devices, col_group)

    def product(left, right, conjugate):
        left_real, left_imag = (left[0], left[1])
        if conjugate:
            left_imag = -left_imag
        real_part = left_real * right[0] - left_imag * right[1]
        imag_part = left_real * right[1] + left_imag * right[0]
        return jnp.stack([real_part, imag_part])

    gated = key_proj * value_proj
    weighted = out_cotangent * query_proj
    slabs = jnp.stack([gated, filter_taps, weighted])
    item_count = slabs.shape[0]
    blocks = slabs.reshape(item_count, channels, run_count, devices, col_group).transpose(
        0, 3, 2, 1, 4
    )
    blocks = blocks.reshape(item_count, devices, run_count, width_cg)
    received = lax.all_to_all(blocks, "seq", split_axis=1, concat_axis=1, tiled=True)
    item_count = received.shape[0]
    flattened = received.reshape(item_count, half_first, width_cg)
    real_sum = jnp.einsum("stm,tk->skm", flattened, cos_first, precision=exact_mode)
    imag_sum = jnp.einsum("stm,tk->skm", flattened, fwd_imag, precision=exact_mode)
    turned_real = real_sum * cos_turn + imag_sum * sin_turn
    turned_imag = imag_sum * cos_turn - real_sum * sin_turn
    stacked = jnp.stack([turned_real, turned_imag], axis=1)
    turned = stacked.reshape(item_count, 2, devices, slot_count, width_cg)
    received = lax.all_to_all(turned, "seq", split_axis=2, concat_axis=2, tiled=True)
    item_count = received.shape[0]
    slots_here = received.shape[3]
    pieces = received.reshape(item_count, 2, devices, slots_here, channels, col_group)

    def contract(values, matrix):
        return jnp.einsum("snkcg,ngq->skcq", values, matrix, precision=exact_mode)

    real_out = contract(pieces[:, 0], cos_grid) + contract(pieces[:, 1], sin_grid)
    imag_out = contract(pieces[:, 1], cos_grid) - contract(pieces[:, 0], sin_grid)
    spectra = jnp.stack([real_out, imag_out], axis=1)
    gated_spec, filter_spec, weighted_spec = (spectra[0], spectra[1], spectra[2])
    forward_prod = product(filter_spec, gated_spec, False)
    grad_list, paired = grad_items(
        product(filter_spec, weighted_spec, True), product(gated_spec, weighted_spec, True)
    )
    spectra = jnp.stack([forward_prod] + grad_list, axis=0)
    item_count = spectra.shape[0]

    def contract(values, matrix):
        return jnp.einsum("skcq,qng->skncg", values, matrix, precision=exact_mode)

    real_out = contract(spectra[:, 0], cos_back) - contract(spectra[:, 1], sin_back)
    imag_out = contract(spectra[:, 0], sin_back) + contract(spectra[:, 1], cos_back)
    columns = jnp.stack([real_out, imag_out], axis=1).reshape(
        item_count, 2, slot_count, devices, width_cg
    )
    received = lax.all_to_all(columns, "seq", split_axis=3, concat_axis=2, tiled=True)
    item_count = received.shape[0]
    flattened = received.reshape(item_count, 2, first_len, width_cg)
    rows_real = flattened[:, 0]
    rows_imag = flattened[:, 1]
    turned_real = rows_real * cos_turn - rows_imag * sin_turn
    turned_imag = rows_imag * cos_turn + rows_real * sin_turn

    def contract(values, matrix):
        return jnp.einsum("skm,tk->stm", values, matrix, precision=exact_mode)

    real_out = contract(turned_real, cos_first) + contract(turned_imag, inv_imag)
    turned = real_out
    item_count = turned.shape[0]
    sending = turned.reshape(item_count, devices, run_count, width_cg)
    returned = lax.all_to_all(sending, "seq", split_axis=1, concat_axis=1, tiled=True)
    returned = returned.reshape(item_count, devices, run_count, channels, col_group).transpose(
        0, 3, 2, 1, 4
    )
    results = returned.reshape(item_count, channels, tokens) * out_scale
    mixed, gated_grad, filter_grad = (results[0], results[1], results[2])
    return (
        query_proj * mixed,
        out_cotangent * mixed,
        gated_grad * value_proj,
        gated_grad * key_proj,
        filter_grad,
    )


def halves(values):
    high = values.astype(jnp.bfloat16)
    return high, (values - high.astype(values.dtype)).astype(jnp.bfloat16)


def transform_tables(rows, scale):
    k1 = np.arange(rows)[:, None] * 2 + 1
    row_angle = -math.pi * ((k1 * np.arange(rows)[None, :]) % (4 * rows)) / (2 * rows)
    row_table = np.concatenate([np.cos(row_angle), np.sin(row_angle)])
    turn_period = 4 * rows * LANES
    turn_angle = -2.0 * math.pi * ((k1 * np.arange(LANES)[None, :]) % turn_period) / turn_period
    turn = np.concatenate([np.cos(turn_angle), np.sin(turn_angle)], axis=1).astype(np.float32)
    lane = np.arange(LANES)
    lane_angle = -2.0 * math.pi * ((lane[:, None] * lane[None, :]) % LANES) / LANES
    cos_lane, sin_lane = (np.cos(lane_angle), np.sin(lane_angle))
    lane_table = np.block([[cos_lane, sin_lane], [-sin_lane, cos_lane]])
    row_high, row_low = halves(row_table)
    back_high, back_low = halves(row_table.T * scale)
    lane_high, lane_low = halves(lane_table)
    return (
        np.concatenate([row_high, row_high, row_low], axis=1),
        turn,
        lane_high,
        lane_low,
        np.concatenate([back_high, back_high, back_low], axis=1),
    )


def pack_kernel(query_ref, key_ref, value_ref, taps_ref, cotangent_ref, out_ref, *, devices, share):
    runs = taps_ref.shape[1] // LANES
    stride = 3 * share * runs
    for c in range(share):
        for r in range(runs):
            at = (pl.ds(c * devices, devices), pl.ds(r * LANES, LANES))
            slabs = (
                key_ref[at] * value_ref[at],
                taps_ref[at],
                cotangent_ref[at] * query_ref[at],
            )
            for a, slab in enumerate(slabs):
                out_ref[pl.ds((a * share + c) * runs + r, devices, stride=stride), :] = slab


def unpack_kernel(
    packed_ref, query_ref, key_ref, value_ref, cotangent_ref,
    out_ref, query_grad_ref, key_grad_ref, value_grad_ref, taps_grad_ref, *, devices, share
):
    runs = query_ref.shape[1] // LANES
    stride = 3 * share * runs
    for c in range(share):
        for r in range(runs):
            at = (pl.ds(c * devices, devices), pl.ds(r * LANES, LANES))
            mixed, gated_grad, taps_grad = (
                packed_ref[pl.ds((a * share + c) * runs + r, devices, stride=stride), :] for a in range(3)
            )
            out_ref[at] = query_ref[at] * mixed
            query_grad_ref[at] = cotangent_ref[at] * mixed
            key_grad_ref[at] = gated_grad * value_ref[at]
            value_grad_ref[at] = gated_grad * key_ref[at]
            taps_grad_ref[at] = taps_grad


def dot(left, right, right_dim=0):
    return lax.dot_general(
        left, right, (((1,), (right_dim,)), ((), ())), preferred_element_type=jnp.float32
    )


def channels_kernel(
    packed_ref, row_ref, turn_ref, lane_high_ref, lane_low_ref, back_ref, out_ref, *, devices, share
):
    items = 3 * share
    runs = packed_ref.shape[0] // (devices * items)
    rows = runs * devices

    def columns(values):
        high, low = halves(values)
        return jnp.concatenate([high, low, high], axis=0)

    def along_lanes(values, right_dim):
        high, low = halves(values)
        lane_high = lane_high_ref[...]
        return (
            dot(high, lane_high, right_dim)
            + dot(low, lane_high, right_dim)
            + dot(high, lane_low_ref[...], right_dim)
        )

    turn_real = turn_ref[:, :LANES]
    turn_imag = turn_ref[:, LANES:]
    sequences = jnp.concatenate(
        [
            jnp.concatenate(
                [packed_ref[pl.ds((s * items + n) * runs, runs), :] for s in range(devices)], axis=0
            )
            for n in range(items)
        ],
        axis=1,
    )
    first = dot(row_ref[...], columns(sequences))
    turned = []
    for n in range(items):
        real = first[:rows, n * LANES : (n + 1) * LANES]
        imag = first[rows:, n * LANES : (n + 1) * LANES]
        turned.append(
            jnp.concatenate(
                [real * turn_real - imag * turn_imag, real * turn_imag + imag * turn_real], axis=1
            )
        )
    spectra = along_lanes(jnp.concatenate(turned, axis=0), 0)
    size = share * rows
    gated, taps, weighted = (
        (spectra[a * size : (a + 1) * size, :LANES], spectra[a * size : (a + 1) * size, LANES:])
        for a in range(3)
    )

    def product(left, right):
        return jnp.concatenate(
            [left[0] * right[0] - left[1] * right[1], left[0] * right[1] + left[1] * right[0]], axis=1
        )

    def against(left, right):
        return jnp.concatenate(
            [left[0] * right[0] + left[1] * right[1], left[0] * right[1] - left[1] * right[0]], axis=1
        )

    spectra = jnp.concatenate(
        [product(taps, gated), against(taps, weighted), against(gated, weighted)], axis=0
    )
    bins = along_lanes(spectra, 1)
    turned = []
    for n in range(items):
        real = bins[n * rows : (n + 1) * rows, :LANES]
        imag = bins[n * rows : (n + 1) * rows, LANES:]
        turned.append(
            jnp.concatenate(
                [real * turn_real + imag * turn_imag, imag * turn_real - real * turn_imag], axis=0
            )
        )
    results = dot(back_ref[...], columns(jnp.concatenate(turned, axis=1)))
    for n in range(items):
        for s in range(devices):
            out_ref[pl.ds((s * items + n) * runs, runs), :] = results[
                s * runs : (s + 1) * runs, n * LANES : (n + 1) * LANES
            ]


def in_vmem(count):
    return [pl.BlockSpec(memory_space=pltpu.VMEM)] * count


def channels_on_devices(query_proj, key_proj, value_proj, filter_taps, out_cotangent):
    devices = lax.axis_size("seq")
    channels, tokens = filter_taps.shape
    share = channels // devices
    rows = tokens * devices // LANES
    full_len = tokens * devices
    scale = 1.0 / (full_len * math.sqrt(full_len))
    packed_shape = jax.ShapeDtypeStruct((channels * 3 * tokens // LANES, LANES), jnp.float32)
    sizes = {"devices": devices, "share": share}

    def call(kernel, outs, *operands):
        many = isinstance(outs, list)
        return pl.pallas_call(
            lambda *refs: kernel(*refs, **sizes),
            name=kernel.__name__,
            out_shape=outs,
            in_specs=in_vmem(len(operands)),
            out_specs=in_vmem(len(outs)) if many else in_vmem(1)[0],
        )(*operands)

    def exchange(packed):
        blocks = packed.reshape(devices, -1, LANES)
        return lax.all_to_all(blocks, "seq", split_axis=0, concat_axis=0, tiled=True).reshape(packed.shape)

    packed = call(pack_kernel, packed_shape, query_proj, key_proj, value_proj, filter_taps, out_cotangent)
    tables = [jnp.asarray(table) for table in transform_tables(rows, scale)]
    results = call(channels_kernel, packed_shape, exchange(packed), *tables)
    outs = [jax.ShapeDtypeStruct((channels, tokens), jnp.float32)] * 5
    return tuple(
        call(unpack_kernel, outs, exchange(results), query_proj, key_proj, value_proj, out_cotangent)
    )


def per_device(query_proj, key_proj, value_proj, filter_taps, out_cotangent):
    devices = lax.axis_size("seq")
    channels, tokens = filter_taps.shape
    owns_channels = channels % devices == 0 and devices % SUBLANES == 0 and tokens % (LANES * SUBLANES) == 0
    plan = channels_on_devices if owns_channels else bins_over_devices
    return plan(query_proj, key_proj, value_proj, filter_taps, out_cotangent)


def solution(mesh):
    placed = (P("ch", "seq"), P("ch", "seq"), P("ch", "seq"), P("ch", "seq"), P("ch", "seq"))
    return jax.shard_map(
        per_device,
        mesh=mesh,
        in_specs=placed,
        out_specs=(P("ch", "seq"), P("ch", "seq"), P("ch", "seq"), P("ch", "seq"), P("ch", "seq")),
        check_vma=False,
    )
```

```python
import math

import jax
import jax.numpy as jnp
import numpy as np
from jax import lax
from jax.experimental import pallas as pl
from jax.experimental.pallas import tpu as pltpu
from jax.sharding import PartitionSpec as P

FAC = 512
LANES = 128
SUBLANES = 8
KERNEL_VMEM = 16 * 2**20


exact_mode = lax.Precision.HIGHEST


def angle_grid(row_ids, col_ids, period):
    angles = (row_ids * col_ids % period).astype(jnp.float32) * (2.0 * math.pi / period)
    return (jnp.cos(angles), jnp.sin(angles))


def index_grid(row_count, col_count):
    return (
        lax.broadcasted_iota(jnp.int32, (row_count, col_count), 0),
        lax.broadcasted_iota(jnp.int32, (row_count, col_count), 1),
    )


def grad_items(first_grad, second_grad):
    return ([first_grad, second_grad], False)


def bins_over_devices(query_proj, key_proj, value_proj, filter_taps, out_cotangent):
    devices = lax.axis_size("seq")
    position = lax.axis_index("seq")
    channels = filter_taps.shape[0]
    tokens = filter_taps.shape[1]
    run_count = tokens // FAC
    half_first = run_count * devices
    first_len = 2 * half_first
    col_group = FAC // devices
    full_len = first_len * FAC
    width_cg = channels * col_group
    out_scale = 1.0 / (full_len * math.sqrt(tokens * devices))
    slot_count = first_len // devices
    time_ids, bin_ids = index_grid(half_first, first_len)
    cos_first, sin_first = angle_grid(time_ids, bin_ids, first_len)
    fwd_imag = -sin_first
    inv_imag = -sin_first
    bin_rows, lane_ids = index_grid(first_len, width_cg)
    cos_turn, sin_turn = angle_grid(bin_rows, position * col_group + lane_ids % col_group, full_len)
    square_rows, square_cols = index_grid(FAC, FAC)
    cos_second, sin_second = angle_grid(square_rows, square_cols, FAC)
    cos_grid = cos_second.reshape(devices, col_group, FAC)
    sin_grid = sin_second.reshape(devices, col_group, FAC)
    cos_back = cos_second.reshape(FAC, devices, col_group)
    sin_back = sin_second.reshape(FAC, devices, col_group)

    def product(left, right, conjugate):
        left_real, left_imag = (left[0], left[1])
        if conjugate:
            left_imag = -left_imag
        real_part = left_real * right[0] - left_imag * right[1]
        imag_part = left_real * right[1] + left_imag * right[0]
        return jnp.stack([real_part, imag_part])

    gated = key_proj * value_proj
    weighted = out_cotangent * query_proj
    slabs = jnp.stack([gated, filter_taps, weighted])
    item_count = slabs.shape[0]
    blocks = slabs.reshape(item_count, channels, run_count, devices, col_group).transpose(
        0, 3, 2, 1, 4
    )
    blocks = blocks.reshape(item_count, devices, run_count, width_cg)
    received = lax.all_to_all(blocks, "seq", split_axis=1, concat_axis=1, tiled=True)
    item_count = received.shape[0]
    flattened = received.reshape(item_count, half_first, width_cg)
    real_sum = jnp.einsum("stm,tk->skm", flattened, cos_first, precision=exact_mode)
    imag_sum = jnp.einsum("stm,tk->skm", flattened, fwd_imag, precision=exact_mode)
    turned_real = real_sum * cos_turn + imag_sum * sin_turn
    turned_imag = imag_sum * cos_turn - real_sum * sin_turn
    stacked = jnp.stack([turned_real, turned_imag], axis=1)
    turned = stacked.reshape(item_count, 2, devices, slot_count, width_cg)
    received = lax.all_to_all(turned, "seq", split_axis=2, concat_axis=2, tiled=True)
    item_count = received.shape[0]
    slots_here = received.shape[3]
    pieces = received.reshape(item_count, 2, devices, slots_here, channels, col_group)

    def contract(values, matrix):
        return jnp.einsum("snkcg,ngq->skcq", values, matrix, precision=exact_mode)

    real_out = contract(pieces[:, 0], cos_grid) + contract(pieces[:, 1], sin_grid)
    imag_out = contract(pieces[:, 1], cos_grid) - contract(pieces[:, 0], sin_grid)
    spectra = jnp.stack([real_out, imag_out], axis=1)
    gated_spec, filter_spec, weighted_spec = (spectra[0], spectra[1], spectra[2])
    forward_prod = product(filter_spec, gated_spec, False)
    grad_list, paired = grad_items(
        product(filter_spec, weighted_spec, True), product(gated_spec, weighted_spec, True)
    )
    spectra = jnp.stack([forward_prod] + grad_list, axis=0)
    item_count = spectra.shape[0]

    def contract(values, matrix):
        return jnp.einsum("skcq,qng->skncg", values, matrix, precision=exact_mode)

    real_out = contract(spectra[:, 0], cos_back) - contract(spectra[:, 1], sin_back)
    imag_out = contract(spectra[:, 0], sin_back) + contract(spectra[:, 1], cos_back)
    columns = jnp.stack([real_out, imag_out], axis=1).reshape(
        item_count, 2, slot_count, devices, width_cg
    )
    received = lax.all_to_all(columns, "seq", split_axis=3, concat_axis=2, tiled=True)
    item_count = received.shape[0]
    flattened = received.reshape(item_count, 2, first_len, width_cg)
    rows_real = flattened[:, 0]
    rows_imag = flattened[:, 1]
    turned_real = rows_real * cos_turn - rows_imag * sin_turn
    turned_imag = rows_imag * cos_turn + rows_real * sin_turn

    def contract(values, matrix):
        return jnp.einsum("skm,tk->stm", values, matrix, precision=exact_mode)

    real_out = contract(turned_real, cos_first) + contract(turned_imag, inv_imag)
    turned = real_out
    item_count = turned.shape[0]
    sending = turned.reshape(item_count, devices, run_count, width_cg)
    returned = lax.all_to_all(sending, "seq", split_axis=1, concat_axis=1, tiled=True)
    returned = returned.reshape(item_count, devices, run_count, channels, col_group).transpose(
        0, 3, 2, 1, 4
    )
    results = returned.reshape(item_count, channels, tokens) * out_scale
    mixed, gated_grad, filter_grad = (results[0], results[1], results[2])
    return (
        query_proj * mixed,
        out_cotangent * mixed,
        gated_grad * value_proj,
        gated_grad * key_proj,
        filter_grad,
    )


def halves(values):
    high = values.astype(jnp.bfloat16)
    return high, (values - high.astype(values.dtype)).astype(jnp.bfloat16)


def transform_tables(rows, scale):
    k1 = np.arange(rows)[:, None] * 2 + 1
    row_angle = -math.pi * ((k1 * np.arange(rows)[None, :]) % (4 * rows)) / (2 * rows)
    row_table = np.concatenate([np.cos(row_angle), np.sin(row_angle)])
    turn_period = 4 * rows * LANES
    turn_angle = -2.0 * math.pi * ((k1 * np.arange(LANES)[None, :]) % turn_period) / turn_period
    turn = np.concatenate([np.cos(turn_angle), np.sin(turn_angle)], axis=1).astype(np.float32)
    lane = np.arange(LANES)
    lane_angle = -2.0 * math.pi * ((lane[:, None] * lane[None, :]) % LANES) / LANES
    cos_lane, sin_lane = (np.cos(lane_angle), np.sin(lane_angle))
    lane_table = np.block([[cos_lane, sin_lane], [-sin_lane, cos_lane]])
    row_high, row_low = halves(row_table)
    back_high, back_low = halves(row_table.T * scale)
    lane_high, lane_low = halves(lane_table)
    return (
        np.concatenate([row_high, row_high, row_low], axis=1),
        turn,
        lane_high,
        lane_low,
        np.concatenate([back_high, back_high, back_low], axis=1),
    )


def pack_kernel(
    query_hbm, key_hbm, value_hbm, taps_hbm, cotangent_hbm, out_ref,
    query_ref, key_ref, value_ref, taps_ref, cotangent_ref, arrived, *, devices, share
):
    copies = [
        pltpu.make_async_copy(source, target, arrived.at[i])
        for i, (source, target) in enumerate(
            (
                (query_hbm, query_ref),
                (key_hbm, key_ref),
                (value_hbm, value_ref),
                (taps_hbm, taps_ref),
                (cotangent_hbm, cotangent_ref),
            )
        )
    ]
    for copy in copies:
        copy.start()
    for copy in copies:
        copy.wait()
    runs = taps_ref.shape[1] // LANES
    stride = 3 * share * runs
    for c in range(share):
        for r in range(runs):
            at = (pl.ds(c * devices, devices), pl.ds(r * LANES, LANES))
            slabs = (
                key_ref[at] * value_ref[at],
                taps_ref[at],
                cotangent_ref[at] * query_ref[at],
            )
            for a, slab in enumerate(slabs):
                out_ref[pl.ds((a * share + c) * runs + r, devices, stride=stride), :] = slab


def unpack_kernel(
    packed_ref, query_ref, key_ref, value_ref, cotangent_ref,
    out_ref, query_grad_ref, key_grad_ref, value_grad_ref, taps_grad_ref, *, devices, share
):
    runs = query_ref.shape[1] // LANES
    stride = 3 * share * runs
    for c in range(share):
        for r in range(runs):
            at = (pl.ds(c * devices, devices), pl.ds(r * LANES, LANES))
            mixed, gated_grad, taps_grad = (
                packed_ref[pl.ds((a * share + c) * runs + r, devices, stride=stride), :] for a in range(3)
            )
            out_ref[at] = query_ref[at] * mixed
            query_grad_ref[at] = cotangent_ref[at] * mixed
            key_grad_ref[at] = gated_grad * value_ref[at]
            value_grad_ref[at] = gated_grad * key_ref[at]
            taps_grad_ref[at] = taps_grad


def dot(left, right, right_dim=0):
    return lax.dot_general(
        left, right, (((1,), (right_dim,)), ((), ())), preferred_element_type=jnp.float32
    )


def channels_kernel(
    packed_ref, row_ref, turn_ref, lane_high_ref, lane_low_ref, back_ref, out_ref, *, devices, share
):
    items = 3 * share
    runs = packed_ref.shape[0] // (devices * items)
    rows = runs * devices

    def columns(values):
        high, low = halves(values)
        return jnp.concatenate([high, low, high], axis=0)

    def along_lanes(values, right_dim):
        high, low = halves(values)
        lane_high = lane_high_ref[...]
        return (
            dot(high, lane_high, right_dim)
            + dot(low, lane_high, right_dim)
            + dot(high, lane_low_ref[...], right_dim)
        )

    turn_real = turn_ref[:, :LANES]
    turn_imag = turn_ref[:, LANES:]
    sequences = jnp.concatenate(
        [
            jnp.concatenate(
                [packed_ref[pl.ds((s * items + n) * runs, runs), :] for s in range(devices)], axis=0
            )
            for n in range(items)
        ],
        axis=1,
    )
    first = dot(row_ref[...], columns(sequences))
    turned = []
    for n in range(items):
        real = first[:rows, n * LANES : (n + 1) * LANES]
        imag = first[rows:, n * LANES : (n + 1) * LANES]
        turned.append(
            jnp.concatenate(
                [real * turn_real - imag * turn_imag, real * turn_imag + imag * turn_real], axis=1
            )
        )
    spectra = along_lanes(jnp.concatenate(turned, axis=0), 0)
    size = share * rows
    gated, taps, weighted = (
        (spectra[a * size : (a + 1) * size, :LANES], spectra[a * size : (a + 1) * size, LANES:])
        for a in range(3)
    )

    def product(left, right):
        return jnp.concatenate(
            [left[0] * right[0] - left[1] * right[1], left[0] * right[1] + left[1] * right[0]], axis=1
        )

    def against(left, right):
        return jnp.concatenate(
            [left[0] * right[0] + left[1] * right[1], left[0] * right[1] - left[1] * right[0]], axis=1
        )

    spectra = jnp.concatenate(
        [product(taps, gated), against(taps, weighted), against(gated, weighted)], axis=0
    )
    bins = along_lanes(spectra, 1)
    turned = []
    for n in range(items):
        real = bins[n * rows : (n + 1) * rows, :LANES]
        imag = bins[n * rows : (n + 1) * rows, LANES:]
        turned.append(
            jnp.concatenate(
                [real * turn_real + imag * turn_imag, imag * turn_real - real * turn_imag], axis=0
            )
        )
    results = dot(back_ref[...], columns(jnp.concatenate(turned, axis=1)))
    for n in range(items):
        for s in range(devices):
            out_ref[pl.ds((s * items + n) * runs, runs), :] = results[
                s * runs : (s + 1) * runs, n * LANES : (n + 1) * LANES
            ]


def in_vmem(count):
    return [pl.BlockSpec(memory_space=pltpu.VMEM)] * count


def channels_on_devices(query_proj, key_proj, value_proj, filter_taps, out_cotangent):
    devices = lax.axis_size("seq")
    channels, tokens = filter_taps.shape
    share = channels // devices
    rows = tokens * devices // LANES
    full_len = tokens * devices
    scale = 1.0 / (full_len * math.sqrt(full_len))
    packed_shape = jax.ShapeDtypeStruct((channels * 3 * tokens // LANES, LANES), jnp.float32)
    sizes = {"devices": devices, "share": share}

    def call(kernel, outs, *operands, space=pltpu.VMEM, scratch=()):
        many = isinstance(outs, list)
        return pl.pallas_call(
            lambda *refs: kernel(*refs, **sizes),
            name=kernel.__name__,
            compiler_params=pltpu.CompilerParams(vmem_limit_bytes=KERNEL_VMEM),
            out_shape=outs,
            in_specs=[pl.BlockSpec(memory_space=space)] * len(operands),
            out_specs=in_vmem(len(outs)) if many else in_vmem(1)[0],
            scratch_shapes=scratch,
        )(*operands)

    def exchange(packed):
        blocks = packed.reshape(devices, -1, LANES)
        return lax.all_to_all(blocks, "seq", split_axis=0, concat_axis=0, tiled=True).reshape(packed.shape)

    inputs = [
        pltpu.with_memory_space_constraint(x, pltpu.HBM)
        for x in (query_proj, key_proj, value_proj, filter_taps, out_cotangent)
    ]
    landing = [pltpu.VMEM((channels, tokens), jnp.float32) for _ in inputs]
    landing.append(pltpu.SemaphoreType.DMA((len(inputs),)))
    packed = call(pack_kernel, packed_shape, *inputs, space=pltpu.HBM, scratch=landing)
    tables = [jnp.asarray(table) for table in transform_tables(rows, scale)]
    results = call(channels_kernel, packed_shape, exchange(packed), *tables)
    outs = [jax.ShapeDtypeStruct((channels, tokens), jnp.float32)] * 5
    return tuple(
        call(unpack_kernel, outs, exchange(results), query_proj, key_proj, value_proj, out_cotangent)
    )


def per_device(query_proj, key_proj, value_proj, filter_taps, out_cotangent):
    devices = lax.axis_size("seq")
    channels, tokens = filter_taps.shape
    owns_channels = channels % devices == 0 and devices % SUBLANES == 0 and tokens % (LANES * SUBLANES) == 0
    plan = channels_on_devices if owns_channels else bins_over_devices
    return plan(query_proj, key_proj, value_proj, filter_taps, out_cotangent)


def solution(mesh):
    placed = (P("ch", "seq"), P("ch", "seq"), P("ch", "seq"), P("ch", "seq"), P("ch", "seq"))
    return jax.shard_map(
        per_device,
        mesh=mesh,
        in_specs=placed,
        out_specs=(P("ch", "seq"), P("ch", "seq"), P("ch", "seq"), P("ch", "seq"), P("ch", "seq")),
        check_vma=False,
    )
```

```python
import math

import jax
import jax.numpy as jnp
import numpy as np
from jax import lax
from jax.experimental import pallas as pl
from jax.experimental.pallas import tpu as pltpu
from jax.sharding import PartitionSpec as P

FAC = 512
LANES = 128
SUBLANES = 8
KERNEL_VMEM = 16 * 2**20


exact_mode = lax.Precision.HIGHEST


def angle_grid(row_ids, col_ids, period):
    angles = (row_ids * col_ids % period).astype(jnp.float32) * (2.0 * math.pi / period)
    return (jnp.cos(angles), jnp.sin(angles))


def index_grid(row_count, col_count):
    return (
        lax.broadcasted_iota(jnp.int32, (row_count, col_count), 0),
        lax.broadcasted_iota(jnp.int32, (row_count, col_count), 1),
    )


def grad_items(first_grad, second_grad):
    return ([first_grad, second_grad], False)


def bins_over_devices(query_proj, key_proj, value_proj, filter_taps, out_cotangent):
    devices = lax.axis_size("seq")
    position = lax.axis_index("seq")
    channels = filter_taps.shape[0]
    tokens = filter_taps.shape[1]
    run_count = tokens // FAC
    half_first = run_count * devices
    first_len = 2 * half_first
    col_group = FAC // devices
    full_len = first_len * FAC
    width_cg = channels * col_group
    out_scale = 1.0 / (full_len * math.sqrt(tokens * devices))
    slot_count = first_len // devices
    time_ids, bin_ids = index_grid(half_first, first_len)
    cos_first, sin_first = angle_grid(time_ids, bin_ids, first_len)
    fwd_imag = -sin_first
    inv_imag = -sin_first
    bin_rows, lane_ids = index_grid(first_len, width_cg)
    cos_turn, sin_turn = angle_grid(bin_rows, position * col_group + lane_ids % col_group, full_len)
    square_rows, square_cols = index_grid(FAC, FAC)
    cos_second, sin_second = angle_grid(square_rows, square_cols, FAC)
    cos_grid = cos_second.reshape(devices, col_group, FAC)
    sin_grid = sin_second.reshape(devices, col_group, FAC)
    cos_back = cos_second.reshape(FAC, devices, col_group)
    sin_back = sin_second.reshape(FAC, devices, col_group)

    def product(left, right, conjugate):
        left_real, left_imag = (left[0], left[1])
        if conjugate:
            left_imag = -left_imag
        real_part = left_real * right[0] - left_imag * right[1]
        imag_part = left_real * right[1] + left_imag * right[0]
        return jnp.stack([real_part, imag_part])

    gated = key_proj * value_proj
    weighted = out_cotangent * query_proj
    slabs = jnp.stack([gated, filter_taps, weighted])
    item_count = slabs.shape[0]
    blocks = slabs.reshape(item_count, channels, run_count, devices, col_group).transpose(
        0, 3, 2, 1, 4
    )
    blocks = blocks.reshape(item_count, devices, run_count, width_cg)
    received = lax.all_to_all(blocks, "seq", split_axis=1, concat_axis=1, tiled=True)
    item_count = received.shape[0]
    flattened = received.reshape(item_count, half_first, width_cg)
    real_sum = jnp.einsum("stm,tk->skm", flattened, cos_first, precision=exact_mode)
    imag_sum = jnp.einsum("stm,tk->skm", flattened, fwd_imag, precision=exact_mode)
    turned_real = real_sum * cos_turn + imag_sum * sin_turn
    turned_imag = imag_sum * cos_turn - real_sum * sin_turn
    stacked = jnp.stack([turned_real, turned_imag], axis=1)
    turned = stacked.reshape(item_count, 2, devices, slot_count, width_cg)
    received = lax.all_to_all(turned, "seq", split_axis=2, concat_axis=2, tiled=True)
    item_count = received.shape[0]
    slots_here = received.shape[3]
    pieces = received.reshape(item_count, 2, devices, slots_here, channels, col_group)

    def contract(values, matrix):
        return jnp.einsum("snkcg,ngq->skcq", values, matrix, precision=exact_mode)

    real_out = contract(pieces[:, 0], cos_grid) + contract(pieces[:, 1], sin_grid)
    imag_out = contract(pieces[:, 1], cos_grid) - contract(pieces[:, 0], sin_grid)
    spectra = jnp.stack([real_out, imag_out], axis=1)
    gated_spec, filter_spec, weighted_spec = (spectra[0], spectra[1], spectra[2])
    forward_prod = product(filter_spec, gated_spec, False)
    grad_list, paired = grad_items(
        product(filter_spec, weighted_spec, True), product(gated_spec, weighted_spec, True)
    )
    spectra = jnp.stack([forward_prod] + grad_list, axis=0)
    item_count = spectra.shape[0]

    def contract(values, matrix):
        return jnp.einsum("skcq,qng->skncg", values, matrix, precision=exact_mode)

    real_out = contract(spectra[:, 0], cos_back) - contract(spectra[:, 1], sin_back)
    imag_out = contract(spectra[:, 0], sin_back) + contract(spectra[:, 1], cos_back)
    columns = jnp.stack([real_out, imag_out], axis=1).reshape(
        item_count, 2, slot_count, devices, width_cg
    )
    received = lax.all_to_all(columns, "seq", split_axis=3, concat_axis=2, tiled=True)
    item_count = received.shape[0]
    flattened = received.reshape(item_count, 2, first_len, width_cg)
    rows_real = flattened[:, 0]
    rows_imag = flattened[:, 1]
    turned_real = rows_real * cos_turn - rows_imag * sin_turn
    turned_imag = rows_imag * cos_turn + rows_real * sin_turn

    def contract(values, matrix):
        return jnp.einsum("skm,tk->stm", values, matrix, precision=exact_mode)

    real_out = contract(turned_real, cos_first) + contract(turned_imag, inv_imag)
    turned = real_out
    item_count = turned.shape[0]
    sending = turned.reshape(item_count, devices, run_count, width_cg)
    returned = lax.all_to_all(sending, "seq", split_axis=1, concat_axis=1, tiled=True)
    returned = returned.reshape(item_count, devices, run_count, channels, col_group).transpose(
        0, 3, 2, 1, 4
    )
    results = returned.reshape(item_count, channels, tokens) * out_scale
    mixed, gated_grad, filter_grad = (results[0], results[1], results[2])
    return (
        query_proj * mixed,
        out_cotangent * mixed,
        gated_grad * value_proj,
        gated_grad * key_proj,
        filter_grad,
    )


def halves(values):
    high = values.astype(jnp.bfloat16)
    return high, (values - high.astype(values.dtype)).astype(jnp.bfloat16)


def transform_tables(rows, scale):
    k1 = np.arange(rows)[:, None] * 2 + 1
    row_angle = -math.pi * ((k1 * np.arange(rows)[None, :]) % (4 * rows)) / (2 * rows)
    row_table = np.concatenate([np.cos(row_angle), np.sin(row_angle)])
    turn_period = 4 * rows * LANES
    turn_angle = -2.0 * math.pi * ((k1 * np.arange(LANES)[None, :]) % turn_period) / turn_period
    turn = np.concatenate([np.cos(turn_angle), np.sin(turn_angle)], axis=1).astype(np.float32)
    lane = np.arange(LANES)
    lane_angle = -2.0 * math.pi * ((lane[:, None] * lane[None, :]) % LANES) / LANES
    cos_lane, sin_lane = (np.cos(lane_angle), np.sin(lane_angle))
    lane_table = np.block([[cos_lane, sin_lane], [-sin_lane, cos_lane]])
    row_high, row_low = halves(row_table)
    back_high, back_low = halves(row_table.T * scale)
    lane_high, lane_low = halves(lane_table)
    return (
        np.concatenate([row_high, row_high, row_low], axis=1),
        turn,
        lane_high,
        lane_low,
        np.concatenate([back_high, back_high, back_low], axis=1),
    )


def exchange_order(devices):
    return [(devices // 2 + 1 - i) % devices for i in range(devices)]


def pack_kernel(
    query_hbm, key_hbm, value_hbm, taps_hbm, cotangent_hbm, out_ref,
    query_ref, key_ref, value_ref, taps_ref, cotangent_ref, arrived, *, devices, share
):
    copies = [
        pltpu.make_async_copy(source, target, arrived.at[i])
        for i, (source, target) in enumerate(
            (
                (query_hbm, query_ref),
                (key_hbm, key_ref),
                (value_hbm, value_ref),
                (taps_hbm, taps_ref),
                (cotangent_hbm, cotangent_ref),
            )
        )
    ]
    for copy in copies:
        copy.start()
    for copy in copies:
        copy.wait()
    runs = taps_ref.shape[1] // LANES
    stride = 3 * share * runs
    for c in range(share):
        for r in range(runs):
            at = (pl.ds(c * devices, devices), pl.ds(r * LANES, LANES))
            slabs = (
                key_ref[at] * value_ref[at],
                taps_ref[at],
                cotangent_ref[at] * query_ref[at],
            )
            for a, slab in enumerate(slabs):
                out_ref[pl.ds((a * share + c) * runs + r, devices, stride=stride), :] = slab


def unpack_kernel(
    packed_ref, query_ref, key_ref, value_ref, cotangent_ref,
    out_ref, query_grad_ref, key_grad_ref, value_grad_ref, taps_grad_ref, *, devices, share
):
    runs = query_ref.shape[1] // LANES
    stride = 3 * share * runs
    for c in range(share):
        for r in range(runs):
            at = (pl.ds(c * devices, devices), pl.ds(r * LANES, LANES))
            mixed, gated_grad, taps_grad = (
                packed_ref[pl.ds((a * share + c) * runs + r, devices, stride=stride), :] for a in range(3)
            )
            out_ref[at] = query_ref[at] * mixed
            query_grad_ref[at] = cotangent_ref[at] * mixed
            key_grad_ref[at] = gated_grad * value_ref[at]
            value_grad_ref[at] = gated_grad * key_ref[at]
            taps_grad_ref[at] = taps_grad


def dot(left, right, right_dim=0):
    return lax.dot_general(
        left, right, (((1,), (right_dim,)), ((), ())), preferred_element_type=jnp.float32
    )


def channels_kernel(
    packed_ref, row_ref, turn_ref, lane_high_ref, lane_low_ref, back_ref, out_ref, *, devices, share
):
    items = 3 * share
    order = exchange_order(devices)
    runs = packed_ref.shape[0] // (devices * items)
    rows = runs * devices

    def columns(values):
        high, low = halves(values)
        return jnp.concatenate([high, low, high], axis=0)

    def along_lanes(values, right_dim):
        high, low = halves(values)
        lane_high = lane_high_ref[...]
        return (
            dot(high, lane_high, right_dim)
            + dot(low, lane_high, right_dim)
            + dot(high, lane_low_ref[...], right_dim)
        )

    turn_real = turn_ref[:, :LANES]
    turn_imag = turn_ref[:, LANES:]
    sequences = jnp.concatenate(
        [
            jnp.concatenate(
                [packed_ref[pl.ds((order.index(s) * items + n) * runs, runs), :] for s in range(devices)],
                axis=0,
            )
            for n in range(items)
        ],
        axis=1,
    )
    first = dot(row_ref[...], columns(sequences))
    turned = []
    for n in range(items):
        real = first[:rows, n * LANES : (n + 1) * LANES]
        imag = first[rows:, n * LANES : (n + 1) * LANES]
        turned.append(
            jnp.concatenate(
                [real * turn_real - imag * turn_imag, real * turn_imag + imag * turn_real], axis=1
            )
        )
    spectra = along_lanes(jnp.concatenate(turned, axis=0), 0)
    size = share * rows
    gated, taps, weighted = (
        (spectra[a * size : (a + 1) * size, :LANES], spectra[a * size : (a + 1) * size, LANES:])
        for a in range(3)
    )

    def product(left, right):
        return jnp.concatenate(
            [left[0] * right[0] - left[1] * right[1], left[0] * right[1] + left[1] * right[0]], axis=1
        )

    def against(left, right):
        return jnp.concatenate(
            [left[0] * right[0] + left[1] * right[1], left[0] * right[1] - left[1] * right[0]], axis=1
        )

    spectra = jnp.concatenate(
        [product(taps, gated), against(taps, weighted), against(gated, weighted)], axis=0
    )
    bins = along_lanes(spectra, 1)
    turned = []
    for n in range(items):
        real = bins[n * rows : (n + 1) * rows, :LANES]
        imag = bins[n * rows : (n + 1) * rows, LANES:]
        turned.append(
            jnp.concatenate(
                [real * turn_real + imag * turn_imag, imag * turn_real - real * turn_imag], axis=0
            )
        )
    results = dot(back_ref[...], columns(jnp.concatenate(turned, axis=1)))
    for n in range(items):
        for s in range(devices):
            out_ref[pl.ds((order.index(s) * items + n) * runs, runs), :] = results[
                s * runs : (s + 1) * runs, n * LANES : (n + 1) * LANES
            ]


def in_vmem(count):
    return [pl.BlockSpec(memory_space=pltpu.VMEM)] * count


def channels_on_devices(query_proj, key_proj, value_proj, filter_taps, out_cotangent):
    devices = lax.axis_size("seq")
    channels, tokens = filter_taps.shape
    share = channels // devices
    rows = tokens * devices // LANES
    full_len = tokens * devices
    scale = 1.0 / (full_len * math.sqrt(full_len))
    packed_shape = jax.ShapeDtypeStruct((channels * 3 * tokens // LANES, LANES), jnp.float32)
    sizes = {"devices": devices, "share": share}

    def call(kernel, outs, *operands, space=pltpu.VMEM, scratch=()):
        many = isinstance(outs, list)
        return pl.pallas_call(
            lambda *refs: kernel(*refs, **sizes),
            name=kernel.__name__,
            compiler_params=pltpu.CompilerParams(vmem_limit_bytes=KERNEL_VMEM),
            out_shape=outs,
            in_specs=[pl.BlockSpec(memory_space=space)] * len(operands),
            out_specs=in_vmem(len(outs)) if many else in_vmem(1)[0],
            scratch_shapes=scratch,
        )(*operands)

    def exchange(packed):
        blocks = packed.reshape(devices, -1, LANES)
        received = lax.all_to_all(
            blocks, "seq", split_axis=0, concat_axis=0, tiled=True, axis_index_groups=[exchange_order(devices)]
        )
        return received.reshape(packed.shape)

    inputs = [
        pltpu.with_memory_space_constraint(x, pltpu.HBM)
        for x in (query_proj, key_proj, value_proj, filter_taps, out_cotangent)
    ]
    landing = [pltpu.VMEM((channels, tokens), jnp.float32) for _ in inputs]
    landing.append(pltpu.SemaphoreType.DMA((len(inputs),)))
    packed = call(pack_kernel, packed_shape, *inputs, space=pltpu.HBM, scratch=landing)
    tables = [jnp.asarray(table) for table in transform_tables(rows, scale)]
    results = call(channels_kernel, packed_shape, exchange(packed), *tables)
    outs = [jax.ShapeDtypeStruct((channels, tokens), jnp.float32)] * 5
    return tuple(
        call(unpack_kernel, outs, exchange(results), query_proj, key_proj, value_proj, out_cotangent)
    )


def per_device(query_proj, key_proj, value_proj, filter_taps, out_cotangent):
    devices = lax.axis_size("seq")
    channels, tokens = filter_taps.shape
    owns_channels = channels % devices == 0 and devices % SUBLANES == 0 and tokens % (LANES * SUBLANES) == 0
    plan = channels_on_devices if owns_channels else bins_over_devices
    return plan(query_proj, key_proj, value_proj, filter_taps, out_cotangent)


def solution(mesh):
    placed = (P("ch", "seq"), P("ch", "seq"), P("ch", "seq"), P("ch", "seq"), P("ch", "seq"))
    return jax.shard_map(
        per_device,
        mesh=mesh,
        in_specs=placed,
        out_specs=(P("ch", "seq"), P("ch", "seq"), P("ch", "seq"), P("ch", "seq"), P("ch", "seq")),
        check_vma=False,
    )
```

```python
import math

import jax
import jax.numpy as jnp
import numpy as np
from jax import lax
from jax.experimental import pallas as pl
from jax.experimental.pallas import tpu as pltpu
from jax.sharding import PartitionSpec as P

FAC = 512
LANES = 128
SUBLANES = 8
KERNEL_VMEM = 16 * 2**20


exact_mode = lax.Precision.HIGHEST


def angle_grid(row_ids, col_ids, period):
    angles = (row_ids * col_ids % period).astype(jnp.float32) * (2.0 * math.pi / period)
    return (jnp.cos(angles), jnp.sin(angles))


def index_grid(row_count, col_count):
    return (
        lax.broadcasted_iota(jnp.int32, (row_count, col_count), 0),
        lax.broadcasted_iota(jnp.int32, (row_count, col_count), 1),
    )


def grad_items(first_grad, second_grad):
    return ([first_grad, second_grad], False)


def bins_over_devices(query_proj, key_proj, value_proj, filter_taps, out_cotangent):
    devices = lax.axis_size("seq")
    position = lax.axis_index("seq")
    channels = filter_taps.shape[0]
    tokens = filter_taps.shape[1]
    run_count = tokens // FAC
    half_first = run_count * devices
    first_len = 2 * half_first
    col_group = FAC // devices
    full_len = first_len * FAC
    width_cg = channels * col_group
    out_scale = 1.0 / (full_len * math.sqrt(tokens * devices))
    slot_count = first_len // devices
    time_ids, bin_ids = index_grid(half_first, first_len)
    cos_first, sin_first = angle_grid(time_ids, bin_ids, first_len)
    fwd_imag = -sin_first
    inv_imag = -sin_first
    bin_rows, lane_ids = index_grid(first_len, width_cg)
    cos_turn, sin_turn = angle_grid(bin_rows, position * col_group + lane_ids % col_group, full_len)
    square_rows, square_cols = index_grid(FAC, FAC)
    cos_second, sin_second = angle_grid(square_rows, square_cols, FAC)
    cos_grid = cos_second.reshape(devices, col_group, FAC)
    sin_grid = sin_second.reshape(devices, col_group, FAC)
    cos_back = cos_second.reshape(FAC, devices, col_group)
    sin_back = sin_second.reshape(FAC, devices, col_group)

    def product(left, right, conjugate):
        left_real, left_imag = (left[0], left[1])
        if conjugate:
            left_imag = -left_imag
        real_part = left_real * right[0] - left_imag * right[1]
        imag_part = left_real * right[1] + left_imag * right[0]
        return jnp.stack([real_part, imag_part])

    gated = key_proj * value_proj
    weighted = out_cotangent * query_proj
    slabs = jnp.stack([gated, filter_taps, weighted])
    item_count = slabs.shape[0]
    blocks = slabs.reshape(item_count, channels, run_count, devices, col_group).transpose(
        0, 3, 2, 1, 4
    )
    blocks = blocks.reshape(item_count, devices, run_count, width_cg)
    received = lax.all_to_all(blocks, "seq", split_axis=1, concat_axis=1, tiled=True)
    item_count = received.shape[0]
    flattened = received.reshape(item_count, half_first, width_cg)
    real_sum = jnp.einsum("stm,tk->skm", flattened, cos_first, precision=exact_mode)
    imag_sum = jnp.einsum("stm,tk->skm", flattened, fwd_imag, precision=exact_mode)
    turned_real = real_sum * cos_turn + imag_sum * sin_turn
    turned_imag = imag_sum * cos_turn - real_sum * sin_turn
    stacked = jnp.stack([turned_real, turned_imag], axis=1)
    turned = stacked.reshape(item_count, 2, devices, slot_count, width_cg)
    received = lax.all_to_all(turned, "seq", split_axis=2, concat_axis=2, tiled=True)
    item_count = received.shape[0]
    slots_here = received.shape[3]
    pieces = received.reshape(item_count, 2, devices, slots_here, channels, col_group)

    def contract(values, matrix):
        return jnp.einsum("snkcg,ngq->skcq", values, matrix, precision=exact_mode)

    real_out = contract(pieces[:, 0], cos_grid) + contract(pieces[:, 1], sin_grid)
    imag_out = contract(pieces[:, 1], cos_grid) - contract(pieces[:, 0], sin_grid)
    spectra = jnp.stack([real_out, imag_out], axis=1)
    gated_spec, filter_spec, weighted_spec = (spectra[0], spectra[1], spectra[2])
    forward_prod = product(filter_spec, gated_spec, False)
    grad_list, paired = grad_items(
        product(filter_spec, weighted_spec, True), product(gated_spec, weighted_spec, True)
    )
    spectra = jnp.stack([forward_prod] + grad_list, axis=0)
    item_count = spectra.shape[0]

    def contract(values, matrix):
        return jnp.einsum("skcq,qng->skncg", values, matrix, precision=exact_mode)

    real_out = contract(spectra[:, 0], cos_back) - contract(spectra[:, 1], sin_back)
    imag_out = contract(spectra[:, 0], sin_back) + contract(spectra[:, 1], cos_back)
    columns = jnp.stack([real_out, imag_out], axis=1).reshape(
        item_count, 2, slot_count, devices, width_cg
    )
    received = lax.all_to_all(columns, "seq", split_axis=3, concat_axis=2, tiled=True)
    item_count = received.shape[0]
    flattened = received.reshape(item_count, 2, first_len, width_cg)
    rows_real = flattened[:, 0]
    rows_imag = flattened[:, 1]
    turned_real = rows_real * cos_turn - rows_imag * sin_turn
    turned_imag = rows_imag * cos_turn + rows_real * sin_turn

    def contract(values, matrix):
        return jnp.einsum("skm,tk->stm", values, matrix, precision=exact_mode)

    real_out = contract(turned_real, cos_first) + contract(turned_imag, inv_imag)
    turned = real_out
    item_count = turned.shape[0]
    sending = turned.reshape(item_count, devices, run_count, width_cg)
    returned = lax.all_to_all(sending, "seq", split_axis=1, concat_axis=1, tiled=True)
    returned = returned.reshape(item_count, devices, run_count, channels, col_group).transpose(
        0, 3, 2, 1, 4
    )
    results = returned.reshape(item_count, channels, tokens) * out_scale
    mixed, gated_grad, filter_grad = (results[0], results[1], results[2])
    return (
        query_proj * mixed,
        out_cotangent * mixed,
        gated_grad * value_proj,
        gated_grad * key_proj,
        filter_grad,
    )


def halves(values):
    high = values.astype(jnp.bfloat16)
    return high, (values - high.astype(values.dtype)).astype(jnp.bfloat16)


def transform_tables(rows, scale):
    k1 = np.arange(rows)[:, None] * 2 + 1
    row_angle = -math.pi * ((k1 * np.arange(rows)[None, :]) % (4 * rows)) / (2 * rows)
    row_table = np.concatenate([np.cos(row_angle), np.sin(row_angle)])
    turn_period = 4 * rows * LANES
    turn_angle = -2.0 * math.pi * ((k1 * np.arange(LANES)[None, :]) % turn_period) / turn_period
    turn = np.concatenate([np.cos(turn_angle), np.sin(turn_angle)], axis=1).astype(np.float32)
    lane = np.arange(LANES)
    lane_angle = -2.0 * math.pi * ((lane[:, None] * lane[None, :]) % LANES) / LANES
    cos_lane, sin_lane = (np.cos(lane_angle), np.sin(lane_angle))
    lane_table = np.block([[cos_lane, sin_lane], [-sin_lane, cos_lane]])
    row_high, row_low = halves(row_table)
    back_high, back_low = halves(row_table.T * scale)
    lane_high, lane_low = halves(lane_table)
    return (
        np.concatenate([row_high, row_high, row_low], axis=1),
        turn,
        lane_high,
        lane_low,
        np.concatenate(
            [np.concatenate([back_high, back_high], axis=1), np.concatenate([back_low, np.zeros_like(back_low)], axis=1)]
        ),
    )


def exchange_order(devices):
    middle = devices // 2 + 1
    order = list(range(middle, -1, -1))
    above = list(range(devices - 1, middle, -1))
    step = len(order) // max(len(above), 1)
    for i, device in enumerate(above):
        order.insert((i + 1) * step + i, device)
    return order


def pack_kernel(
    query_hbm, key_hbm, value_hbm, taps_hbm, cotangent_hbm, out_ref,
    query_ref, key_ref, value_ref, taps_ref, cotangent_ref, arrived, *, devices, share
):
    sources = (query_hbm, key_hbm, value_hbm, taps_hbm, cotangent_hbm)
    targets = (query_ref, key_ref, value_ref, taps_ref, cotangent_ref)
    copies = [
        [
            pltpu.make_async_copy(
                source.at[pl.ds(c * devices, devices)], target.at[pl.ds(c * devices, devices)], arrived.at[c, i]
            )
            for i, (source, target) in enumerate(zip(sources, targets))
        ]
        for c in range(share)
    ]
    for group in copies:
        for copy in group:
            copy.start()
    runs = taps_ref.shape[1] // LANES
    stride = 3 * share * runs
    for c in range(share):
        for copy in copies[c]:
            copy.wait()
        for r in range(runs):
            at = (pl.ds(c * devices, devices), pl.ds(r * LANES, LANES))
            slabs = (
                key_ref[at] * value_ref[at],
                taps_ref[at],
                cotangent_ref[at] * query_ref[at],
            )
            for a, slab in enumerate(slabs):
                out_ref[pl.ds((a * share + c) * runs + r, devices, stride=stride), :] = slab


def unpack_kernel(
    packed_ref, query_ref, key_ref, value_ref, cotangent_ref,
    out_ref, query_grad_ref, key_grad_ref, value_grad_ref, taps_grad_ref, *, devices, share
):
    runs = query_ref.shape[1] // LANES
    stride = 3 * share * runs
    for c in range(share):
        for r in range(runs):
            at = (pl.ds(c * devices, devices), pl.ds(r * LANES, LANES))
            mixed, gated_grad, taps_grad = (
                packed_ref[pl.ds((a * share + c) * runs + r, devices, stride=stride), :] for a in range(3)
            )
            out_ref[at] = query_ref[at] * mixed
            query_grad_ref[at] = cotangent_ref[at] * mixed
            key_grad_ref[at] = gated_grad * value_ref[at]
            value_grad_ref[at] = gated_grad * key_ref[at]
            taps_grad_ref[at] = taps_grad


def dot(left, right, right_dim=0):
    return lax.dot_general(
        left, right, (((1,), (right_dim,)), ((), ())), preferred_element_type=jnp.float32
    )


def channels_kernel(
    packed_ref, row_ref, turn_ref, lane_high_ref, lane_low_ref, back_ref, out_ref, *, devices, share
):
    items = 3 * share
    order = exchange_order(devices)
    runs = packed_ref.shape[0] // (devices * items)
    rows = runs * devices

    def columns(values):
        high, low = halves(values)
        return jnp.concatenate([high, low, high], axis=0)

    def along_lanes(values, right_dim):
        high, low = halves(values)
        size = values.shape[0]
        both = dot(jnp.concatenate([high, low], axis=0), lane_high_ref[...], right_dim)
        return both[:size] + both[size:] + dot(high, lane_low_ref[...], right_dim)

    turn_real = turn_ref[:, :LANES]
    turn_imag = turn_ref[:, LANES:]
    sequences = jnp.concatenate(
        [
            jnp.concatenate(
                [packed_ref[pl.ds((order.index(s) * items + n) * runs, runs), :] for s in range(devices)],
                axis=0,
            )
            for n in range(items)
        ],
        axis=1,
    )
    first = dot(row_ref[...], columns(sequences))
    turned = []
    for n in range(items):
        real = first[:rows, n * LANES : (n + 1) * LANES]
        imag = first[rows:, n * LANES : (n + 1) * LANES]
        turned.append(
            jnp.concatenate(
                [real * turn_real - imag * turn_imag, real * turn_imag + imag * turn_real], axis=1
            )
        )
    spectra = along_lanes(jnp.concatenate(turned, axis=0), 0)
    size = share * rows
    gated, taps, weighted = (
        (spectra[a * size : (a + 1) * size, :LANES], spectra[a * size : (a + 1) * size, LANES:])
        for a in range(3)
    )

    def product(left, right):
        return jnp.concatenate(
            [left[0] * right[0] - left[1] * right[1], left[0] * right[1] + left[1] * right[0]], axis=1
        )

    def against(left, right):
        return jnp.concatenate(
            [left[0] * right[0] + left[1] * right[1], left[0] * right[1] - left[1] * right[0]], axis=1
        )

    spectra = jnp.concatenate(
        [product(taps, gated), against(taps, weighted), against(gated, weighted)], axis=0
    )
    bins = along_lanes(spectra, 1)
    turned = []
    for n in range(items):
        real = bins[n * rows : (n + 1) * rows, :LANES]
        imag = bins[n * rows : (n + 1) * rows, LANES:]
        turned.append(
            jnp.concatenate(
                [real * turn_real + imag * turn_imag, imag * turn_real - real * turn_imag], axis=0
            )
        )
    high, low = halves(jnp.concatenate(turned, axis=1))
    both = dot(back_ref[...], jnp.concatenate([high, low], axis=0))
    results = both[:rows] + both[rows:]
    for n in range(items):
        for s in range(devices):
            out_ref[pl.ds((order.index(s) * items + n) * runs, runs), :] = results[
                s * runs : (s + 1) * runs, n * LANES : (n + 1) * LANES
            ]


def in_vmem(count):
    return [pl.BlockSpec(memory_space=pltpu.VMEM)] * count


def channels_on_devices(query_proj, key_proj, value_proj, filter_taps, out_cotangent):
    devices = lax.axis_size("seq")
    channels, tokens = filter_taps.shape
    share = channels // devices
    rows = tokens * devices // LANES
    full_len = tokens * devices
    scale = 1.0 / (full_len * math.sqrt(full_len))
    packed_shape = jax.ShapeDtypeStruct((channels * 3 * tokens // LANES, LANES), jnp.float32)
    sizes = {"devices": devices, "share": share}

    def call(kernel, outs, *operands, space=pltpu.VMEM, scratch=()):
        many = isinstance(outs, list)
        return pl.pallas_call(
            lambda *refs: kernel(*refs, **sizes),
            name=kernel.__name__,
            compiler_params=pltpu.CompilerParams(vmem_limit_bytes=KERNEL_VMEM),
            out_shape=outs,
            in_specs=[pl.BlockSpec(memory_space=space)] * len(operands),
            out_specs=in_vmem(len(outs)) if many else in_vmem(1)[0],
            scratch_shapes=scratch,
        )(*operands)

    def exchange(packed):
        blocks = packed.reshape(devices, -1, LANES)
        received = lax.all_to_all(
            blocks, "seq", split_axis=0, concat_axis=0, tiled=True, axis_index_groups=[exchange_order(devices)]
        )
        return received.reshape(packed.shape)

    inputs = [
        pltpu.with_memory_space_constraint(x, pltpu.HBM)
        for x in (query_proj, key_proj, value_proj, filter_taps, out_cotangent)
    ]
    landing = [pltpu.VMEM((channels, tokens), jnp.float32) for _ in inputs]
    landing.append(pltpu.SemaphoreType.DMA((share, len(inputs))))
    packed = call(pack_kernel, packed_shape, *inputs, space=pltpu.HBM, scratch=landing)
    tables = [jnp.asarray(table) for table in transform_tables(rows, scale)]
    results = call(channels_kernel, packed_shape, exchange(packed), *tables)
    outs = [jax.ShapeDtypeStruct((channels, tokens), jnp.float32)] * 5
    return tuple(
        call(unpack_kernel, outs, exchange(results), query_proj, key_proj, value_proj, out_cotangent)
    )


def per_device(query_proj, key_proj, value_proj, filter_taps, out_cotangent):
    devices = lax.axis_size("seq")
    channels, tokens = filter_taps.shape
    owns_channels = channels % devices == 0 and devices % SUBLANES == 0 and tokens % (LANES * SUBLANES) == 0
    plan = channels_on_devices if owns_channels else bins_over_devices
    return plan(query_proj, key_proj, value_proj, filter_taps, out_cotangent)


def solution(mesh):
    placed = (P("ch", "seq"), P("ch", "seq"), P("ch", "seq"), P("ch", "seq"), P("ch", "seq"))
    return jax.shard_map(
        per_device,
        mesh=mesh,
        in_specs=placed,
        out_specs=(P("ch", "seq"), P("ch", "seq"), P("ch", "seq"), P("ch", "seq"), P("ch", "seq")),
        check_vma=False,
    )
```

```python
import math

import jax
import jax.numpy as jnp
import numpy as np
from jax import lax
from jax.experimental import pallas as pl
from jax.experimental.pallas import tpu as pltpu
from jax.sharding import PartitionSpec as P

FAC = 512
LANES = 128
SUBLANES = 8
KERNEL_VMEM = 16 * 2**20


exact_mode = lax.Precision.HIGHEST


def angle_grid(row_ids, col_ids, period):
    angles = (row_ids * col_ids % period).astype(jnp.float32) * (2.0 * math.pi / period)
    return (jnp.cos(angles), jnp.sin(angles))


def index_grid(row_count, col_count):
    return (
        lax.broadcasted_iota(jnp.int32, (row_count, col_count), 0),
        lax.broadcasted_iota(jnp.int32, (row_count, col_count), 1),
    )


def grad_items(first_grad, second_grad):
    return ([first_grad, second_grad], False)


def bins_over_devices(query_proj, key_proj, value_proj, filter_taps, out_cotangent):
    devices = lax.axis_size("seq")
    position = lax.axis_index("seq")
    channels = filter_taps.shape[0]
    tokens = filter_taps.shape[1]
    run_count = tokens // FAC
    half_first = run_count * devices
    first_len = 2 * half_first
    col_group = FAC // devices
    full_len = first_len * FAC
    width_cg = channels * col_group
    out_scale = 1.0 / (full_len * math.sqrt(tokens * devices))
    slot_count = first_len // devices
    time_ids, bin_ids = index_grid(half_first, first_len)
    cos_first, sin_first = angle_grid(time_ids, bin_ids, first_len)
    fwd_imag = -sin_first
    inv_imag = -sin_first
    bin_rows, lane_ids = index_grid(first_len, width_cg)
    cos_turn, sin_turn = angle_grid(bin_rows, position * col_group + lane_ids % col_group, full_len)
    square_rows, square_cols = index_grid(FAC, FAC)
    cos_second, sin_second = angle_grid(square_rows, square_cols, FAC)
    cos_grid = cos_second.reshape(devices, col_group, FAC)
    sin_grid = sin_second.reshape(devices, col_group, FAC)
    cos_back = cos_second.reshape(FAC, devices, col_group)
    sin_back = sin_second.reshape(FAC, devices, col_group)

    def product(left, right, conjugate):
        left_real, left_imag = (left[0], left[1])
        if conjugate:
            left_imag = -left_imag
        real_part = left_real * right[0] - left_imag * right[1]
        imag_part = left_real * right[1] + left_imag * right[0]
        return jnp.stack([real_part, imag_part])

    gated = key_proj * value_proj
    weighted = out_cotangent * query_proj
    slabs = jnp.stack([gated, filter_taps, weighted])
    item_count = slabs.shape[0]
    blocks = slabs.reshape(item_count, channels, run_count, devices, col_group).transpose(
        0, 3, 2, 1, 4
    )
    blocks = blocks.reshape(item_count, devices, run_count, width_cg)
    received = lax.all_to_all(blocks, "seq", split_axis=1, concat_axis=1, tiled=True)
    item_count = received.shape[0]
    flattened = received.reshape(item_count, half_first, width_cg)
    real_sum = jnp.einsum("stm,tk->skm", flattened, cos_first, precision=exact_mode)
    imag_sum = jnp.einsum("stm,tk->skm", flattened, fwd_imag, precision=exact_mode)
    turned_real = real_sum * cos_turn + imag_sum * sin_turn
    turned_imag = imag_sum * cos_turn - real_sum * sin_turn
    stacked = jnp.stack([turned_real, turned_imag], axis=1)
    turned = stacked.reshape(item_count, 2, devices, slot_count, width_cg)
    received = lax.all_to_all(turned, "seq", split_axis=2, concat_axis=2, tiled=True)
    item_count = received.shape[0]
    slots_here = received.shape[3]
    pieces = received.reshape(item_count, 2, devices, slots_here, channels, col_group)

    def contract(values, matrix):
        return jnp.einsum("snkcg,ngq->skcq", values, matrix, precision=exact_mode)

    real_out = contract(pieces[:, 0], cos_grid) + contract(pieces[:, 1], sin_grid)
    imag_out = contract(pieces[:, 1], cos_grid) - contract(pieces[:, 0], sin_grid)
    spectra = jnp.stack([real_out, imag_out], axis=1)
    gated_spec, filter_spec, weighted_spec = (spectra[0], spectra[1], spectra[2])
    forward_prod = product(filter_spec, gated_spec, False)
    grad_list, paired = grad_items(
        product(filter_spec, weighted_spec, True), product(gated_spec, weighted_spec, True)
    )
    spectra = jnp.stack([forward_prod] + grad_list, axis=0)
    item_count = spectra.shape[0]

    def contract(values, matrix):
        return jnp.einsum("skcq,qng->skncg", values, matrix, precision=exact_mode)

    real_out = contract(spectra[:, 0], cos_back) - contract(spectra[:, 1], sin_back)
    imag_out = contract(spectra[:, 0], sin_back) + contract(spectra[:, 1], cos_back)
    columns = jnp.stack([real_out, imag_out], axis=1).reshape(
        item_count, 2, slot_count, devices, width_cg
    )
    received = lax.all_to_all(columns, "seq", split_axis=3, concat_axis=2, tiled=True)
    item_count = received.shape[0]
    flattened = received.reshape(item_count, 2, first_len, width_cg)
    rows_real = flattened[:, 0]
    rows_imag = flattened[:, 1]
    turned_real = rows_real * cos_turn - rows_imag * sin_turn
    turned_imag = rows_imag * cos_turn + rows_real * sin_turn

    def contract(values, matrix):
        return jnp.einsum("skm,tk->stm", values, matrix, precision=exact_mode)

    real_out = contract(turned_real, cos_first) + contract(turned_imag, inv_imag)
    turned = real_out
    item_count = turned.shape[0]
    sending = turned.reshape(item_count, devices, run_count, width_cg)
    returned = lax.all_to_all(sending, "seq", split_axis=1, concat_axis=1, tiled=True)
    returned = returned.reshape(item_count, devices, run_count, channels, col_group).transpose(
        0, 3, 2, 1, 4
    )
    results = returned.reshape(item_count, channels, tokens) * out_scale
    mixed, gated_grad, filter_grad = (results[0], results[1], results[2])
    return (
        query_proj * mixed,
        out_cotangent * mixed,
        gated_grad * value_proj,
        gated_grad * key_proj,
        filter_grad,
    )


def halves(values):
    high = values.astype(jnp.bfloat16)
    return high, (values - high.astype(values.dtype)).astype(jnp.bfloat16)


def transform_tables(rows, scale):
    k1 = np.arange(rows)[:, None] * 2 + 1
    row_angle = -math.pi * ((k1 * np.arange(rows)[None, :]) % (4 * rows)) / (2 * rows)
    row_table = np.concatenate([np.cos(row_angle), np.sin(row_angle)])
    turn_period = 4 * rows * LANES
    turn_angle = -2.0 * math.pi * ((k1 * np.arange(LANES)[None, :]) % turn_period) / turn_period
    turn = np.concatenate([np.cos(turn_angle), np.sin(turn_angle)], axis=1).astype(np.float32)
    lane = np.arange(LANES)
    lane_angle = -2.0 * math.pi * ((lane[:, None] * lane[None, :]) % LANES) / LANES
    cos_lane, sin_lane = (np.cos(lane_angle), np.sin(lane_angle))
    lane_table = np.block([[cos_lane, sin_lane], [-sin_lane, cos_lane]])
    row_high, row_low = halves(row_table)
    back_high, back_low = halves(row_table.T * scale)
    lane_high, lane_low = halves(lane_table)
    return (
        np.concatenate([row_high, row_high, row_low], axis=1),
        turn,
        lane_high,
        lane_low,
        np.concatenate(
            [np.concatenate([back_high, back_high], axis=1), np.concatenate([back_low, np.zeros_like(back_low)], axis=1)]
        ),
    )


def exchange_order(devices):
    middle = min(devices // 2 + 1, devices - 1)
    order = list(range(middle, -1, -1))
    above = list(range(devices - 1, middle, -1))
    step = len(order) // max(len(above), 1)
    for i, device in enumerate(above):
        order.insert((i + 1) * step + i, device)
    return order


def pack_kernel(
    query_hbm, key_hbm, value_hbm, taps_hbm, cotangent_hbm,
    packed_ref, query_ref, key_ref, value_ref, cotangent_ref, taps_ref, arrived, *, devices, share
):
    sources = (query_hbm, key_hbm, value_hbm, taps_hbm, cotangent_hbm)
    targets = (query_ref, key_ref, value_ref, taps_ref, cotangent_ref)
    copies = [
        [
            pltpu.make_async_copy(
                source.at[pl.ds(c * devices, devices)], target.at[pl.ds(c * devices, devices)], arrived.at[c, i]
            )
            for i, (source, target) in enumerate(zip(sources, targets))
        ]
        for c in range(share)
    ]
    for group in copies:
        for copy in group:
            copy.start()
    runs = taps_ref.shape[1] // LANES
    stride = 3 * share * runs
    for c in range(share):
        for copy in copies[c]:
            copy.wait()
        for r in range(runs):
            at = (pl.ds(c * devices, devices), pl.ds(r * LANES, LANES))
            slabs = (
                key_ref[at] * value_ref[at],
                taps_ref[at],
                cotangent_ref[at] * query_ref[at],
            )
            for a, slab in enumerate(slabs):
                packed_ref[pl.ds((a * share + c) * runs + r, devices, stride=stride), :] = slab


def unpack_kernel(
    packed_ref, query_ref, key_ref, value_ref, cotangent_ref,
    out_ref, query_grad_ref, key_grad_ref, value_grad_ref, taps_grad_ref, *, devices, share
):
    runs = query_ref.shape[1] // LANES
    stride = 3 * share * runs
    for c in range(share):
        for r in range(runs):
            at = (pl.ds(c * devices, devices), pl.ds(r * LANES, LANES))
            mixed, gated_grad, taps_grad = (
                packed_ref[pl.ds((a * share + c) * runs + r, devices, stride=stride), :] for a in range(3)
            )
            out_ref[at] = query_ref[at] * mixed
            query_grad_ref[at] = cotangent_ref[at] * mixed
            key_grad_ref[at] = gated_grad * value_ref[at]
            value_grad_ref[at] = gated_grad * key_ref[at]
            taps_grad_ref[at] = taps_grad


def dot(left, right, right_dim=0):
    return lax.dot_general(
        left, right, (((1,), (right_dim,)), ((), ())), preferred_element_type=jnp.float32
    )


def channels_kernel(
    packed_ref, row_ref, turn_ref, lane_high_ref, lane_low_ref, back_ref, out_ref, *, devices, share
):
    items = 3 * share
    order = exchange_order(devices)
    runs = packed_ref.shape[0] // (devices * items)
    rows = runs * devices

    def columns(values):
        high, low = halves(values)
        return jnp.concatenate([high, low, high], axis=0)

    def along_lanes(values, right_dim):
        high, low = halves(values)
        size = values.shape[0]
        both = dot(jnp.concatenate([high, low], axis=0), lane_high_ref[...], right_dim)
        return both[:size] + both[size:] + dot(high, lane_low_ref[...], right_dim)

    turn_real = turn_ref[:, :LANES]
    turn_imag = turn_ref[:, LANES:]
    sequences = jnp.concatenate(
        [
            jnp.concatenate(
                [packed_ref[pl.ds((order.index(s) * items + n) * runs, runs), :] for s in range(devices)],
                axis=0,
            )
            for n in range(items)
        ],
        axis=1,
    )
    first = dot(row_ref[...], columns(sequences))
    turned = []
    for n in range(items):
        real = first[:rows, n * LANES : (n + 1) * LANES]
        imag = first[rows:, n * LANES : (n + 1) * LANES]
        turned.append(
            jnp.concatenate(
                [real * turn_real - imag * turn_imag, real * turn_imag + imag * turn_real], axis=1
            )
        )
    spectra = along_lanes(jnp.concatenate(turned, axis=0), 0)
    size = share * rows
    gated, taps, weighted = (
        (spectra[a * size : (a + 1) * size, :LANES], spectra[a * size : (a + 1) * size, LANES:])
        for a in range(3)
    )

    def product(left, right):
        return jnp.concatenate(
            [left[0] * right[0] - left[1] * right[1], left[0] * right[1] + left[1] * right[0]], axis=1
        )

    def against(left, right):
        return jnp.concatenate(
            [left[0] * right[0] + left[1] * right[1], left[0] * right[1] - left[1] * right[0]], axis=1
        )

    spectra = jnp.concatenate(
        [product(taps, gated), against(taps, weighted), against(gated, weighted)], axis=0
    )
    bins = along_lanes(spectra, 1)
    turned = []
    for n in range(items):
        real = bins[n * rows : (n + 1) * rows, :LANES]
        imag = bins[n * rows : (n + 1) * rows, LANES:]
        turned.append(
            jnp.concatenate(
                [real * turn_real + imag * turn_imag, imag * turn_real - real * turn_imag], axis=0
            )
        )
    high, low = halves(jnp.concatenate(turned, axis=1))
    both = dot(back_ref[...], jnp.concatenate([high, low], axis=0))
    results = both[:rows] + both[rows:]
    for n in range(items):
        for s in range(devices):
            out_ref[pl.ds((order.index(s) * items + n) * runs, runs), :] = results[
                s * runs : (s + 1) * runs, n * LANES : (n + 1) * LANES
            ]


def in_vmem(count):
    return [pl.BlockSpec(memory_space=pltpu.VMEM)] * count


def channels_on_devices(query_proj, key_proj, value_proj, filter_taps, out_cotangent):
    devices = lax.axis_size("seq")
    channels, tokens = filter_taps.shape
    share = channels // devices
    rows = tokens * devices // LANES
    full_len = tokens * devices
    scale = 1.0 / (full_len * math.sqrt(full_len))
    packed_shape = jax.ShapeDtypeStruct((channels * 3 * tokens // LANES, LANES), jnp.float32)
    shape = jax.ShapeDtypeStruct((channels, tokens), jnp.float32)
    sizes = {"devices": devices, "share": share}

    def call(kernel, outs, *operands, space=pltpu.VMEM, scratch=()):
        many = isinstance(outs, list)
        return pl.pallas_call(
            lambda *refs: kernel(*refs, **sizes),
            name=kernel.__name__,
            compiler_params=pltpu.CompilerParams(vmem_limit_bytes=KERNEL_VMEM),
            out_shape=outs,
            in_specs=[pl.BlockSpec(memory_space=space)] * len(operands),
            out_specs=in_vmem(len(outs)) if many else in_vmem(1)[0],
            scratch_shapes=scratch,
        )(*operands)

    def exchange(packed):
        blocks = packed.reshape(devices, -1, LANES)
        received = lax.all_to_all(
            blocks, "seq", split_axis=0, concat_axis=0, tiled=True, axis_index_groups=[exchange_order(devices)]
        )
        return received.reshape(packed.shape)

    inputs = [
        pltpu.with_memory_space_constraint(x, pltpu.HBM)
        for x in (query_proj, key_proj, value_proj, filter_taps, out_cotangent)
    ]
    packed, *gates = call(
        pack_kernel,
        [packed_shape, *[shape] * 4],
        *inputs,
        space=pltpu.HBM,
        scratch=[pltpu.VMEM((channels, tokens), jnp.float32), pltpu.SemaphoreType.DMA((share, len(inputs)))],
    )
    tables = [jnp.asarray(table) for table in transform_tables(rows, scale)]
    results = call(channels_kernel, packed_shape, exchange(packed), *tables)
    return tuple(call(unpack_kernel, [shape] * 5, exchange(results), *gates))


def per_device(query_proj, key_proj, value_proj, filter_taps, out_cotangent):
    devices = lax.axis_size("seq")
    channels, tokens = filter_taps.shape
    owns_channels = channels % devices == 0 and devices % SUBLANES == 0 and tokens % (LANES * SUBLANES) == 0
    plan = channels_on_devices if owns_channels else bins_over_devices
    return plan(query_proj, key_proj, value_proj, filter_taps, out_cotangent)


def solution(mesh):
    placed = (P("ch", "seq"), P("ch", "seq"), P("ch", "seq"), P("ch", "seq"), P("ch", "seq"))
    return jax.shard_map(
        per_device,
        mesh=mesh,
        in_specs=placed,
        out_specs=(P("ch", "seq"), P("ch", "seq"), P("ch", "seq"), P("ch", "seq"), P("ch", "seq")),
        check_vma=False,
    )
```

```python
import math

import jax
import jax.numpy as jnp
import numpy as np
from jax import lax
from jax.experimental import pallas as pl
from jax.experimental.pallas import tpu as pltpu
from jax.sharding import PartitionSpec as P

FAC = 512
LANES = 128
SUBLANES = 8
KERNEL_VMEM = 16 * 2**20


exact_mode = lax.Precision.HIGHEST


def angle_grid(row_ids, col_ids, period):
    angles = (row_ids * col_ids % period).astype(jnp.float32) * (2.0 * math.pi / period)
    return (jnp.cos(angles), jnp.sin(angles))


def index_grid(row_count, col_count):
    return (
        lax.broadcasted_iota(jnp.int32, (row_count, col_count), 0),
        lax.broadcasted_iota(jnp.int32, (row_count, col_count), 1),
    )


def grad_items(first_grad, second_grad):
    return ([first_grad, second_grad], False)


def bins_over_devices(query_proj, key_proj, value_proj, filter_taps, out_cotangent):
    devices = lax.axis_size("seq")
    position = lax.axis_index("seq")
    channels = filter_taps.shape[0]
    tokens = filter_taps.shape[1]
    run_count = tokens // FAC
    half_first = run_count * devices
    first_len = 2 * half_first
    col_group = FAC // devices
    full_len = first_len * FAC
    width_cg = channels * col_group
    out_scale = 1.0 / (full_len * math.sqrt(tokens * devices))
    slot_count = first_len // devices
    time_ids, bin_ids = index_grid(half_first, first_len)
    cos_first, sin_first = angle_grid(time_ids, bin_ids, first_len)
    fwd_imag = -sin_first
    inv_imag = -sin_first
    bin_rows, lane_ids = index_grid(first_len, width_cg)
    cos_turn, sin_turn = angle_grid(bin_rows, position * col_group + lane_ids % col_group, full_len)
    square_rows, square_cols = index_grid(FAC, FAC)
    cos_second, sin_second = angle_grid(square_rows, square_cols, FAC)
    cos_grid = cos_second.reshape(devices, col_group, FAC)
    sin_grid = sin_second.reshape(devices, col_group, FAC)
    cos_back = cos_second.reshape(FAC, devices, col_group)
    sin_back = sin_second.reshape(FAC, devices, col_group)

    def product(left, right, conjugate):
        left_real, left_imag = (left[0], left[1])
        if conjugate:
            left_imag = -left_imag
        real_part = left_real * right[0] - left_imag * right[1]
        imag_part = left_real * right[1] + left_imag * right[0]
        return jnp.stack([real_part, imag_part])

    gated = key_proj * value_proj
    weighted = out_cotangent * query_proj
    slabs = jnp.stack([gated, filter_taps, weighted])
    item_count = slabs.shape[0]
    blocks = slabs.reshape(item_count, channels, run_count, devices, col_group).transpose(
        0, 3, 2, 1, 4
    )
    blocks = blocks.reshape(item_count, devices, run_count, width_cg)
    received = lax.all_to_all(blocks, "seq", split_axis=1, concat_axis=1, tiled=True)
    item_count = received.shape[0]
    flattened = received.reshape(item_count, half_first, width_cg)
    real_sum = jnp.einsum("stm,tk->skm", flattened, cos_first, precision=exact_mode)
    imag_sum = jnp.einsum("stm,tk->skm", flattened, fwd_imag, precision=exact_mode)
    turned_real = real_sum * cos_turn + imag_sum * sin_turn
    turned_imag = imag_sum * cos_turn - real_sum * sin_turn
    stacked = jnp.stack([turned_real, turned_imag], axis=1)
    turned = stacked.reshape(item_count, 2, devices, slot_count, width_cg)
    received = lax.all_to_all(turned, "seq", split_axis=2, concat_axis=2, tiled=True)
    item_count = received.shape[0]
    slots_here = received.shape[3]
    pieces = received.reshape(item_count, 2, devices, slots_here, channels, col_group)

    def contract(values, matrix):
        return jnp.einsum("snkcg,ngq->skcq", values, matrix, precision=exact_mode)

    real_out = contract(pieces[:, 0], cos_grid) + contract(pieces[:, 1], sin_grid)
    imag_out = contract(pieces[:, 1], cos_grid) - contract(pieces[:, 0], sin_grid)
    spectra = jnp.stack([real_out, imag_out], axis=1)
    gated_spec, filter_spec, weighted_spec = (spectra[0], spectra[1], spectra[2])
    forward_prod = product(filter_spec, gated_spec, False)
    grad_list, paired = grad_items(
        product(filter_spec, weighted_spec, True), product(gated_spec, weighted_spec, True)
    )
    spectra = jnp.stack([forward_prod] + grad_list, axis=0)
    item_count = spectra.shape[0]

    def contract(values, matrix):
        return jnp.einsum("skcq,qng->skncg", values, matrix, precision=exact_mode)

    real_out = contract(spectra[:, 0], cos_back) - contract(spectra[:, 1], sin_back)
    imag_out = contract(spectra[:, 0], sin_back) + contract(spectra[:, 1], cos_back)
    columns = jnp.stack([real_out, imag_out], axis=1).reshape(
        item_count, 2, slot_count, devices, width_cg
    )
    received = lax.all_to_all(columns, "seq", split_axis=3, concat_axis=2, tiled=True)
    item_count = received.shape[0]
    flattened = received.reshape(item_count, 2, first_len, width_cg)
    rows_real = flattened[:, 0]
    rows_imag = flattened[:, 1]
    turned_real = rows_real * cos_turn - rows_imag * sin_turn
    turned_imag = rows_imag * cos_turn + rows_real * sin_turn

    def contract(values, matrix):
        return jnp.einsum("skm,tk->stm", values, matrix, precision=exact_mode)

    real_out = contract(turned_real, cos_first) + contract(turned_imag, inv_imag)
    turned = real_out
    item_count = turned.shape[0]
    sending = turned.reshape(item_count, devices, run_count, width_cg)
    returned = lax.all_to_all(sending, "seq", split_axis=1, concat_axis=1, tiled=True)
    returned = returned.reshape(item_count, devices, run_count, channels, col_group).transpose(
        0, 3, 2, 1, 4
    )
    results = returned.reshape(item_count, channels, tokens) * out_scale
    mixed, gated_grad, filter_grad = (results[0], results[1], results[2])
    return (
        query_proj * mixed,
        out_cotangent * mixed,
        gated_grad * value_proj,
        gated_grad * key_proj,
        filter_grad,
    )


def halves(values):
    high = values.astype(jnp.bfloat16)
    return high, (values - high.astype(values.dtype)).astype(jnp.bfloat16)


def transform_tables(rows, scale):
    k1 = np.arange(rows)[:, None] * 2 + 1
    row_angle = -math.pi * ((k1 * np.arange(rows)[None, :]) % (4 * rows)) / (2 * rows)
    row_table = np.concatenate([np.cos(row_angle), np.sin(row_angle)])
    turn_period = 4 * rows * LANES
    turn_angle = -2.0 * math.pi * ((k1 * np.arange(LANES)[None, :]) % turn_period) / turn_period
    turn = np.concatenate([np.cos(turn_angle), np.sin(turn_angle)], axis=1).astype(np.float32)
    lane = np.arange(LANES)
    lane_angle = -2.0 * math.pi * ((lane[:, None] * lane[None, :]) % LANES) / LANES
    cos_lane, sin_lane = (np.cos(lane_angle), np.sin(lane_angle))
    lane_table = np.block([[cos_lane, sin_lane], [-sin_lane, cos_lane]])
    row_high, row_low = halves(row_table)
    back_high, back_low = halves(row_table.T * scale)
    lane_high, lane_low = halves(lane_table)
    return (
        np.concatenate([row_high, row_high, row_low], axis=1),
        turn,
        lane_high,
        lane_low,
        np.concatenate(
            [np.concatenate([back_high, back_high], axis=1), np.concatenate([back_low, np.zeros_like(back_low)], axis=1)]
        ),
    )


def exchange_order(devices):
    middle = min(devices // 2 + 1, devices - 1)
    order = list(range(middle, -1, -1))
    above = list(range(devices - 1, middle, -1))
    step = len(order) // max(len(above), 1)
    for i, device in enumerate(above):
        order.insert((i + 1) * step + i, device)
    return order


def pack_kernel(
    query_hbm, key_hbm, value_hbm, taps_hbm, cotangent_hbm,
    packed_ref, query_ref, key_ref, value_ref, cotangent_ref, taps_ref, arrived, *, devices, share
):
    sources = (query_hbm, key_hbm, value_hbm, taps_hbm, cotangent_hbm)
    targets = (query_ref, key_ref, value_ref, taps_ref, cotangent_ref)
    copies = [
        [
            pltpu.make_async_copy(
                source.at[pl.ds(c * devices, devices)], target.at[pl.ds(c * devices, devices)], arrived.at[c, i]
            )
            for i, (source, target) in enumerate(zip(sources, targets))
        ]
        for c in range(share)
    ]
    for group in copies:
        for copy in group:
            copy.start()
    runs = taps_ref.shape[1] // LANES
    stride = 3 * share * runs
    for c in range(share):
        for copy in copies[c]:
            copy.wait()
        for r in range(runs):
            at = (pl.ds(c * devices, devices), pl.ds(r * LANES, LANES))
            slabs = (
                key_ref[at] * value_ref[at],
                taps_ref[at],
                cotangent_ref[at] * query_ref[at],
            )
            for a, slab in enumerate(slabs):
                packed_ref[pl.ds((a * share + c) * runs + r, devices, stride=stride), :] = slab


def unpack_kernel(
    packed_ref, query_ref, key_ref, value_ref, cotangent_ref,
    out_ref, query_grad_ref, key_grad_ref, value_grad_ref, taps_grad_ref, *, devices, share
):
    runs = query_ref.shape[1] // LANES
    stride = 3 * share * runs
    for c in range(share):
        for r in range(runs):
            at = (pl.ds(c * devices, devices), pl.ds(r * LANES, LANES))
            mixed, gated_grad, taps_grad = (
                packed_ref[pl.ds((a * share + c) * runs + r, devices, stride=stride), :] for a in range(3)
            )
            out_ref[at] = query_ref[at] * mixed
            query_grad_ref[at] = cotangent_ref[at] * mixed
            key_grad_ref[at] = gated_grad * value_ref[at]
            value_grad_ref[at] = gated_grad * key_ref[at]
            taps_grad_ref[at] = taps_grad


def dot(left, right, right_dim=0):
    return lax.dot_general(
        left, right, (((1,), (right_dim,)), ((), ())), preferred_element_type=jnp.float32
    )


def channels_kernel(
    packed_ref, row_ref, turn_ref, lane_high_ref, lane_low_ref, back_ref, out_ref, *, devices, share
):
    items = 3 * share
    order = exchange_order(devices)
    runs = packed_ref.shape[0] // (devices * items)
    rows = runs * devices

    def columns(values):
        high, low = halves(values)
        return jnp.concatenate([high, low, high], axis=0)

    def along_lanes(values, right_dim):
        high, low = halves(values)
        size = values.shape[0]
        both = dot(jnp.concatenate([high, low], axis=0), lane_high_ref[...], right_dim)
        return both[:size] + both[size:] + dot(high, lane_low_ref[...], right_dim)

    turn_real = turn_ref[:, :LANES]
    turn_imag = turn_ref[:, LANES:]
    def product(left, right):
        return jnp.concatenate(
            [left[0] * right[0] - left[1] * right[1], left[0] * right[1] + left[1] * right[0]], axis=1
        )

    def against(left, right):
        return jnp.concatenate(
            [left[0] * right[0] + left[1] * right[1], left[0] * right[1] - left[1] * right[0]], axis=1
        )

    def first_of(a):
        sequences = jnp.concatenate(
            [
                jnp.concatenate(
                    [packed_ref[pl.ds((order.index(s) * items + n) * runs, runs), :] for s in range(devices)],
                    axis=0,
                )
                for n in range(a * share, (a + 1) * share)
            ],
            axis=1,
        )
        return dot(row_ref[...], columns(sequences))

    def lines_of(first):
        turned = []
        for c in range(share):
            real = first[:rows, c * LANES : (c + 1) * LANES]
            imag = first[rows:, c * LANES : (c + 1) * LANES]
            turned.append(
                jnp.concatenate(
                    [real * turn_real - imag * turn_imag, real * turn_imag + imag * turn_real], axis=1
                )
            )
        lines = along_lanes(jnp.concatenate(turned, axis=0), 0)
        return lines[:, :LANES], lines[:, LANES:]

    def results_of(bins):
        turned = []
        for c in range(share):
            real = bins[c * rows : (c + 1) * rows, :LANES]
            imag = bins[c * rows : (c + 1) * rows, LANES:]
            turned.append(
                jnp.concatenate(
                    [real * turn_real + imag * turn_imag, imag * turn_real - real * turn_imag], axis=0
                )
            )
        high, low = halves(jnp.concatenate(turned, axis=1))
        return dot(back_ref[...], jnp.concatenate([high, low], axis=0))

    def store(a, both):
        results = both[:rows] + both[rows:]
        for c in range(share):
            for s in range(devices):
                out_ref[pl.ds((order.index(s) * items + a * share + c) * runs, runs), :] = results[
                    s * runs : (s + 1) * runs, c * LANES : (c + 1) * LANES
                ]

    firsts = [first_of(a) for a in range(3)]
    gated, taps, weighted = [lines_of(first) for first in firsts]
    spectra = (product(taps, gated), against(taps, weighted), against(gated, weighted))
    bins = [along_lanes(spectrum, 1) for spectrum in spectra]
    results = [results_of(values) for values in bins]
    for a, both in enumerate(results):
        store(a, both)


def in_vmem(count):
    return [pl.BlockSpec(memory_space=pltpu.VMEM)] * count


def channels_on_devices(query_proj, key_proj, value_proj, filter_taps, out_cotangent):
    devices = lax.axis_size("seq")
    channels, tokens = filter_taps.shape
    share = channels // devices
    rows = tokens * devices // LANES
    full_len = tokens * devices
    scale = 1.0 / (full_len * math.sqrt(full_len))
    packed_shape = jax.ShapeDtypeStruct((channels * 3 * tokens // LANES, LANES), jnp.float32)
    shape = jax.ShapeDtypeStruct((channels, tokens), jnp.float32)
    sizes = {"devices": devices, "share": share}

    def call(kernel, outs, *operands, space=pltpu.VMEM, scratch=()):
        many = isinstance(outs, list)
        return pl.pallas_call(
            lambda *refs: kernel(*refs, **sizes),
            name=kernel.__name__,
            compiler_params=pltpu.CompilerParams(vmem_limit_bytes=KERNEL_VMEM),
            out_shape=outs,
            in_specs=[pl.BlockSpec(memory_space=space)] * len(operands),
            out_specs=in_vmem(len(outs)) if many else in_vmem(1)[0],
            scratch_shapes=scratch,
        )(*operands)

    def exchange(packed):
        blocks = packed.reshape(devices, -1, LANES)
        received = lax.all_to_all(
            blocks, "seq", split_axis=0, concat_axis=0, tiled=True, axis_index_groups=[exchange_order(devices)]
        )
        return received.reshape(packed.shape)

    inputs = [
        pltpu.with_memory_space_constraint(x, pltpu.HBM)
        for x in (query_proj, key_proj, value_proj, filter_taps, out_cotangent)
    ]
    packed, *gates = call(
        pack_kernel,
        [packed_shape, *[shape] * 4],
        *inputs,
        space=pltpu.HBM,
        scratch=[pltpu.VMEM((channels, tokens), jnp.float32), pltpu.SemaphoreType.DMA((share, len(inputs)))],
    )
    tables = [jnp.asarray(table) for table in transform_tables(rows, scale)]
    results = call(channels_kernel, packed_shape, exchange(packed), *tables)
    return tuple(call(unpack_kernel, [shape] * 5, exchange(results), *gates))


def per_device(query_proj, key_proj, value_proj, filter_taps, out_cotangent):
    devices = lax.axis_size("seq")
    channels, tokens = filter_taps.shape
    owns_channels = channels % devices == 0 and devices % SUBLANES == 0 and tokens % (LANES * SUBLANES) == 0
    plan = channels_on_devices if owns_channels else bins_over_devices
    return plan(query_proj, key_proj, value_proj, filter_taps, out_cotangent)


def solution(mesh):
    placed = (P("ch", "seq"), P("ch", "seq"), P("ch", "seq"), P("ch", "seq"), P("ch", "seq"))
    return jax.shard_map(
        per_device,
        mesh=mesh,
        in_specs=placed,
        out_specs=(P("ch", "seq"), P("ch", "seq"), P("ch", "seq"), P("ch", "seq"), P("ch", "seq")),
        check_vma=False,
    )
```

```python
import math

import jax
import jax.numpy as jnp
import numpy as np
from jax import lax
from jax.experimental import pallas as pl
from jax.experimental.pallas import tpu as pltpu
from jax.sharding import PartitionSpec as P

FAC = 512
LANES = 128
SUBLANES = 8
KERNEL_VMEM = 16 * 2**20


exact_mode = lax.Precision.HIGHEST


def angle_grid(row_ids, col_ids, period):
    angles = (row_ids * col_ids % period).astype(jnp.float32) * (2.0 * math.pi / period)
    return (jnp.cos(angles), jnp.sin(angles))


def index_grid(row_count, col_count):
    return (
        lax.broadcasted_iota(jnp.int32, (row_count, col_count), 0),
        lax.broadcasted_iota(jnp.int32, (row_count, col_count), 1),
    )


def grad_items(first_grad, second_grad):
    return ([first_grad, second_grad], False)


def bins_over_devices(query_proj, key_proj, value_proj, filter_taps, out_cotangent):
    devices = lax.axis_size("seq")
    position = lax.axis_index("seq")
    channels = filter_taps.shape[0]
    tokens = filter_taps.shape[1]
    run_count = tokens // FAC
    half_first = run_count * devices
    first_len = 2 * half_first
    col_group = FAC // devices
    full_len = first_len * FAC
    width_cg = channels * col_group
    out_scale = 1.0 / (full_len * math.sqrt(tokens * devices))
    slot_count = first_len // devices
    time_ids, bin_ids = index_grid(half_first, first_len)
    cos_first, sin_first = angle_grid(time_ids, bin_ids, first_len)
    fwd_imag = -sin_first
    inv_imag = -sin_first
    bin_rows, lane_ids = index_grid(first_len, width_cg)
    cos_turn, sin_turn = angle_grid(bin_rows, position * col_group + lane_ids % col_group, full_len)
    square_rows, square_cols = index_grid(FAC, FAC)
    cos_second, sin_second = angle_grid(square_rows, square_cols, FAC)
    cos_grid = cos_second.reshape(devices, col_group, FAC)
    sin_grid = sin_second.reshape(devices, col_group, FAC)
    cos_back = cos_second.reshape(FAC, devices, col_group)
    sin_back = sin_second.reshape(FAC, devices, col_group)

    def product(left, right, conjugate):
        left_real, left_imag = (left[0], left[1])
        if conjugate:
            left_imag = -left_imag
        real_part = left_real * right[0] - left_imag * right[1]
        imag_part = left_real * right[1] + left_imag * right[0]
        return jnp.stack([real_part, imag_part])

    gated = key_proj * value_proj
    weighted = out_cotangent * query_proj
    slabs = jnp.stack([gated, filter_taps, weighted])
    item_count = slabs.shape[0]
    blocks = slabs.reshape(item_count, channels, run_count, devices, col_group).transpose(
        0, 3, 2, 1, 4
    )
    blocks = blocks.reshape(item_count, devices, run_count, width_cg)
    received = lax.all_to_all(blocks, "seq", split_axis=1, concat_axis=1, tiled=True)
    item_count = received.shape[0]
    flattened = received.reshape(item_count, half_first, width_cg)
    real_sum = jnp.einsum("stm,tk->skm", flattened, cos_first, precision=exact_mode)
    imag_sum = jnp.einsum("stm,tk->skm", flattened, fwd_imag, precision=exact_mode)
    turned_real = real_sum * cos_turn + imag_sum * sin_turn
    turned_imag = imag_sum * cos_turn - real_sum * sin_turn
    stacked = jnp.stack([turned_real, turned_imag], axis=1)
    turned = stacked.reshape(item_count, 2, devices, slot_count, width_cg)
    received = lax.all_to_all(turned, "seq", split_axis=2, concat_axis=2, tiled=True)
    item_count = received.shape[0]
    slots_here = received.shape[3]
    pieces = received.reshape(item_count, 2, devices, slots_here, channels, col_group)

    def contract(values, matrix):
        return jnp.einsum("snkcg,ngq->skcq", values, matrix, precision=exact_mode)

    real_out = contract(pieces[:, 0], cos_grid) + contract(pieces[:, 1], sin_grid)
    imag_out = contract(pieces[:, 1], cos_grid) - contract(pieces[:, 0], sin_grid)
    spectra = jnp.stack([real_out, imag_out], axis=1)
    gated_spec, filter_spec, weighted_spec = (spectra[0], spectra[1], spectra[2])
    forward_prod = product(filter_spec, gated_spec, False)
    grad_list, paired = grad_items(
        product(filter_spec, weighted_spec, True), product(gated_spec, weighted_spec, True)
    )
    spectra = jnp.stack([forward_prod] + grad_list, axis=0)
    item_count = spectra.shape[0]

    def contract(values, matrix):
        return jnp.einsum("skcq,qng->skncg", values, matrix, precision=exact_mode)

    real_out = contract(spectra[:, 0], cos_back) - contract(spectra[:, 1], sin_back)
    imag_out = contract(spectra[:, 0], sin_back) + contract(spectra[:, 1], cos_back)
    columns = jnp.stack([real_out, imag_out], axis=1).reshape(
        item_count, 2, slot_count, devices, width_cg
    )
    received = lax.all_to_all(columns, "seq", split_axis=3, concat_axis=2, tiled=True)
    item_count = received.shape[0]
    flattened = received.reshape(item_count, 2, first_len, width_cg)
    rows_real = flattened[:, 0]
    rows_imag = flattened[:, 1]
    turned_real = rows_real * cos_turn - rows_imag * sin_turn
    turned_imag = rows_imag * cos_turn + rows_real * sin_turn

    def contract(values, matrix):
        return jnp.einsum("skm,tk->stm", values, matrix, precision=exact_mode)

    real_out = contract(turned_real, cos_first) + contract(turned_imag, inv_imag)
    turned = real_out
    item_count = turned.shape[0]
    sending = turned.reshape(item_count, devices, run_count, width_cg)
    returned = lax.all_to_all(sending, "seq", split_axis=1, concat_axis=1, tiled=True)
    returned = returned.reshape(item_count, devices, run_count, channels, col_group).transpose(
        0, 3, 2, 1, 4
    )
    results = returned.reshape(item_count, channels, tokens) * out_scale
    mixed, gated_grad, filter_grad = (results[0], results[1], results[2])
    return (
        query_proj * mixed,
        out_cotangent * mixed,
        gated_grad * value_proj,
        gated_grad * key_proj,
        filter_grad,
    )


def halves(values):
    high = values.astype(jnp.bfloat16)
    return high, (values - high.astype(values.dtype)).astype(jnp.bfloat16)


def transform_tables(rows, scale):
    k1 = np.arange(rows)[:, None] * 2 + 1
    row_angle = -math.pi * ((k1 * np.arange(rows)[None, :]) % (4 * rows)) / (2 * rows)
    row_table = np.concatenate([np.cos(row_angle), np.sin(row_angle)])
    turn_period = 4 * rows * LANES
    turn_angle = -2.0 * math.pi * ((k1 * np.arange(LANES)[None, :]) % turn_period) / turn_period
    turn = np.concatenate([np.cos(turn_angle), np.sin(turn_angle)], axis=1).astype(np.float32)
    lane = np.arange(LANES)
    lane_angle = -2.0 * math.pi * ((lane[:, None] * lane[None, :]) % LANES) / LANES
    cos_lane, sin_lane = (np.cos(lane_angle), np.sin(lane_angle))
    lane_table = np.concatenate([cos_lane, sin_lane], axis=1)
    row_high, row_low = halves(row_table)
    back_high, back_low = halves(row_table.T * scale)
    lane_high, lane_low = halves(lane_table)
    return (
        np.concatenate([row_high, row_high, row_low], axis=1),
        turn,
        lane_high,
        lane_low,
        np.concatenate(
            [np.concatenate([back_high, back_high], axis=1), np.concatenate([back_low, np.zeros_like(back_low)], axis=1)]
        ),
    )


def exchange_order(devices):
    eighth = devices // 8
    return [part * eighth + i for part in (5, 2, 3, 7, 1, 4, 0, 6) for i in range(eighth)]


def pack_kernel(
    query_hbm, key_hbm, value_hbm, taps_hbm, cotangent_hbm,
    packed_ref, query_ref, key_ref, value_ref, cotangent_ref, taps_ref, arrived, *, devices, share
):
    sources = (query_hbm, key_hbm, value_hbm, taps_hbm, cotangent_hbm)
    targets = (query_ref, key_ref, value_ref, taps_ref, cotangent_ref)
    copies = [
        [
            pltpu.make_async_copy(
                source.at[pl.ds(c * devices, devices)], target.at[pl.ds(c * devices, devices)], arrived.at[c, i]
            )
            for i, (source, target) in enumerate(zip(sources, targets))
        ]
        for c in range(share)
    ]
    for group in copies:
        for copy in group:
            copy.start()
    runs = taps_ref.shape[1] // LANES
    stride = 3 * share * runs
    for c in range(share):
        for copy in copies[c]:
            copy.wait()
        for r in range(runs):
            at = (pl.ds(c * devices, devices), pl.ds(r * LANES, LANES))
            slabs = (
                key_ref[at] * value_ref[at],
                taps_ref[at],
                cotangent_ref[at] * query_ref[at],
            )
            for a, slab in enumerate(slabs):
                packed_ref[pl.ds((a * share + c) * runs + r, devices, stride=stride), :] = slab


def unpack_kernel(
    packed_ref, query_ref, key_ref, value_ref, cotangent_ref,
    out_ref, query_grad_ref, key_grad_ref, value_grad_ref, taps_grad_ref, *, devices, share
):
    runs = query_ref.shape[1] // LANES
    stride = 3 * share * runs
    for c in range(share):
        for r in range(runs):
            at = (pl.ds(c * devices, devices), pl.ds(r * LANES, LANES))
            mixed, gated_grad, taps_grad = (
                packed_ref[pl.ds((a * share + c) * runs + r, devices, stride=stride), :] for a in range(3)
            )
            out_ref[at] = query_ref[at] * mixed
            query_grad_ref[at] = cotangent_ref[at] * mixed
            key_grad_ref[at] = gated_grad * value_ref[at]
            value_grad_ref[at] = gated_grad * key_ref[at]
            taps_grad_ref[at] = taps_grad


def dot(left, right, right_dim=0):
    return lax.dot_general(
        left, right, (((1,), (right_dim,)), ((), ())), preferred_element_type=jnp.float32
    )


def channels_kernel(
    packed_ref, row_ref, turn_ref, lane_high_ref, lane_low_ref, back_ref, out_ref, *, devices, share
):
    items = 3 * share
    order = exchange_order(devices)
    runs = packed_ref.shape[0] // (devices * items)
    rows = runs * devices

    def columns(values):
        high, low = halves(values)
        return jnp.concatenate([high, low, high], axis=0)

    def along_lanes(values, high_table, low_table):
        high, low = halves(values)
        size = values.shape[0]
        both = dot(jnp.concatenate([high, low], axis=0), high_table)
        return both[:size] + both[size:] + dot(high, low_table)

    def square(table_ref, conjugate):
        cosines, sines = (table_ref[:, :LANES], table_ref[:, LANES:])
        above, below = (-sines, sines) if conjugate else (sines, -sines)
        return jnp.concatenate(
            [jnp.concatenate([cosines, above], axis=1), jnp.concatenate([below, cosines], axis=1)], axis=0
        )

    forward = (square(lane_high_ref, False), square(lane_low_ref, False))
    backward = (square(lane_high_ref, True), square(lane_low_ref, True))
    turn_real = turn_ref[:, :LANES]
    turn_imag = turn_ref[:, LANES:]
    def product(left, right):
        return jnp.concatenate(
            [left[0] * right[0] - left[1] * right[1], left[0] * right[1] + left[1] * right[0]], axis=1
        )

    def against(left, right):
        return jnp.concatenate(
            [left[0] * right[0] + left[1] * right[1], left[0] * right[1] - left[1] * right[0]], axis=1
        )

    def first_of(a):
        sequences = jnp.concatenate(
            [
                jnp.concatenate(
                    [packed_ref[pl.ds((order.index(s) * items + n) * runs, runs), :] for s in range(devices)],
                    axis=0,
                )
                for n in range(a * share, (a + 1) * share)
            ],
            axis=1,
        )
        return dot(row_ref[...], columns(sequences))

    def lines_of(first):
        turned = []
        for c in range(share):
            real = first[:rows, c * LANES : (c + 1) * LANES]
            imag = first[rows:, c * LANES : (c + 1) * LANES]
            turned.append(
                jnp.concatenate(
                    [real * turn_real - imag * turn_imag, real * turn_imag + imag * turn_real], axis=1
                )
            )
        lines = along_lanes(jnp.concatenate(turned, axis=0), *forward)
        return lines[:, :LANES], lines[:, LANES:]

    def results_of(bins):
        turned = []
        for c in range(share):
            real = bins[c * rows : (c + 1) * rows, :LANES]
            imag = bins[c * rows : (c + 1) * rows, LANES:]
            turned.append(
                jnp.concatenate(
                    [real * turn_real + imag * turn_imag, imag * turn_real - real * turn_imag], axis=0
                )
            )
        high, low = halves(jnp.concatenate(turned, axis=1))
        return dot(back_ref[...], jnp.concatenate([high, low], axis=0))

    def store(a, both):
        results = both[:rows] + both[rows:]
        for c in range(share):
            for s in range(devices):
                out_ref[pl.ds((order.index(s) * items + a * share + c) * runs, runs), :] = results[
                    s * runs : (s + 1) * runs, c * LANES : (c + 1) * LANES
                ]

    firsts = [first_of(a) for a in range(3)]
    gated, taps, weighted = [lines_of(first) for first in firsts]
    spectra = (product(taps, gated), against(taps, weighted), against(gated, weighted))
    bins = [along_lanes(spectrum, *backward) for spectrum in spectra]
    results = [results_of(values) for values in bins]
    for a, both in enumerate(results):
        store(a, both)


def in_vmem(count):
    return [pl.BlockSpec(memory_space=pltpu.VMEM)] * count


def channels_on_devices(query_proj, key_proj, value_proj, filter_taps, out_cotangent):
    devices = lax.axis_size("seq")
    channels, tokens = filter_taps.shape
    share = channels // devices
    rows = tokens * devices // LANES
    full_len = tokens * devices
    scale = 1.0 / (full_len * math.sqrt(full_len))
    packed_shape = jax.ShapeDtypeStruct((channels * 3 * tokens // LANES, LANES), jnp.float32)
    shape = jax.ShapeDtypeStruct((channels, tokens), jnp.float32)
    sizes = {"devices": devices, "share": share}

    def call(kernel, outs, *operands, space=pltpu.VMEM, scratch=()):
        many = isinstance(outs, list)
        return pl.pallas_call(
            lambda *refs: kernel(*refs, **sizes),
            name=kernel.__name__,
            compiler_params=pltpu.CompilerParams(vmem_limit_bytes=KERNEL_VMEM),
            out_shape=outs,
            in_specs=[pl.BlockSpec(memory_space=space)] * len(operands),
            out_specs=in_vmem(len(outs)) if many else in_vmem(1)[0],
            scratch_shapes=scratch,
        )(*operands)

    def exchange(packed):
        blocks = packed.reshape(devices, -1, LANES)
        received = lax.all_to_all(
            blocks, "seq", split_axis=0, concat_axis=0, tiled=True, axis_index_groups=[exchange_order(devices)]
        )
        return received.reshape(packed.shape)

    inputs = [
        pltpu.with_memory_space_constraint(x, pltpu.HBM)
        for x in (query_proj, key_proj, value_proj, filter_taps, out_cotangent)
    ]
    packed, *gates = call(
        pack_kernel,
        [packed_shape, *[shape] * 4],
        *inputs,
        space=pltpu.HBM,
        scratch=[pltpu.VMEM((channels, tokens), jnp.float32), pltpu.SemaphoreType.DMA((share, len(inputs)))],
    )
    tables = [jnp.asarray(table) for table in transform_tables(rows, scale)]
    results = call(channels_kernel, packed_shape, exchange(packed), *tables)
    return tuple(call(unpack_kernel, [shape] * 5, exchange(results), *gates))


def per_device(query_proj, key_proj, value_proj, filter_taps, out_cotangent):
    devices = lax.axis_size("seq")
    channels, tokens = filter_taps.shape
    owns_channels = channels % devices == 0 and devices % SUBLANES == 0 and tokens % (LANES * SUBLANES) == 0
    plan = channels_on_devices if owns_channels else bins_over_devices
    return plan(query_proj, key_proj, value_proj, filter_taps, out_cotangent)


def solution(mesh):
    placed = (P("ch", "seq"), P("ch", "seq"), P("ch", "seq"), P("ch", "seq"), P("ch", "seq"))
    return jax.shard_map(
        per_device,
        mesh=mesh,
        in_specs=placed,
        out_specs=(P("ch", "seq"), P("ch", "seq"), P("ch", "seq"), P("ch", "seq"), P("ch", "seq")),
        check_vma=False,
    )
```

```python
import math

import jax
import jax.numpy as jnp
import numpy as np
from jax import lax
from jax.experimental import pallas as pl
from jax.experimental.pallas import tpu as pltpu
from jax.sharding import PartitionSpec as P

FAC = 512
LANES = 128
SUBLANES = 8
KERNEL_VMEM = 16 * 2**20


exact_mode = lax.Precision.HIGHEST


def angle_grid(row_ids, col_ids, period):
    angles = (row_ids * col_ids % period).astype(jnp.float32) * (2.0 * math.pi / period)
    return (jnp.cos(angles), jnp.sin(angles))


def index_grid(row_count, col_count):
    return (
        lax.broadcasted_iota(jnp.int32, (row_count, col_count), 0),
        lax.broadcasted_iota(jnp.int32, (row_count, col_count), 1),
    )


def grad_items(first_grad, second_grad):
    return ([first_grad, second_grad], False)


def bins_over_devices(query_proj, key_proj, value_proj, filter_taps, out_cotangent):
    devices = lax.axis_size("seq")
    position = lax.axis_index("seq")
    channels = filter_taps.shape[0]
    tokens = filter_taps.shape[1]
    run_count = tokens // FAC
    half_first = run_count * devices
    first_len = 2 * half_first
    col_group = FAC // devices
    full_len = first_len * FAC
    width_cg = channels * col_group
    out_scale = 1.0 / (full_len * math.sqrt(tokens * devices))
    slot_count = first_len // devices
    time_ids, bin_ids = index_grid(half_first, first_len)
    cos_first, sin_first = angle_grid(time_ids, bin_ids, first_len)
    fwd_imag = -sin_first
    inv_imag = -sin_first
    bin_rows, lane_ids = index_grid(first_len, width_cg)
    cos_turn, sin_turn = angle_grid(bin_rows, position * col_group + lane_ids % col_group, full_len)
    square_rows, square_cols = index_grid(FAC, FAC)
    cos_second, sin_second = angle_grid(square_rows, square_cols, FAC)
    cos_grid = cos_second.reshape(devices, col_group, FAC)
    sin_grid = sin_second.reshape(devices, col_group, FAC)
    cos_back = cos_second.reshape(FAC, devices, col_group)
    sin_back = sin_second.reshape(FAC, devices, col_group)

    def product(left, right, conjugate):
        left_real, left_imag = (left[0], left[1])
        if conjugate:
            left_imag = -left_imag
        real_part = left_real * right[0] - left_imag * right[1]
        imag_part = left_real * right[1] + left_imag * right[0]
        return jnp.stack([real_part, imag_part])

    gated = key_proj * value_proj
    weighted = out_cotangent * query_proj
    slabs = jnp.stack([gated, filter_taps, weighted])
    item_count = slabs.shape[0]
    blocks = slabs.reshape(item_count, channels, run_count, devices, col_group).transpose(
        0, 3, 2, 1, 4
    )
    blocks = blocks.reshape(item_count, devices, run_count, width_cg)
    received = lax.all_to_all(blocks, "seq", split_axis=1, concat_axis=1, tiled=True)
    item_count = received.shape[0]
    flattened = received.reshape(item_count, half_first, width_cg)
    real_sum = jnp.einsum("stm,tk->skm", flattened, cos_first, precision=exact_mode)
    imag_sum = jnp.einsum("stm,tk->skm", flattened, fwd_imag, precision=exact_mode)
    turned_real = real_sum * cos_turn + imag_sum * sin_turn
    turned_imag = imag_sum * cos_turn - real_sum * sin_turn
    stacked = jnp.stack([turned_real, turned_imag], axis=1)
    turned = stacked.reshape(item_count, 2, devices, slot_count, width_cg)
    received = lax.all_to_all(turned, "seq", split_axis=2, concat_axis=2, tiled=True)
    item_count = received.shape[0]
    slots_here = received.shape[3]
    pieces = received.reshape(item_count, 2, devices, slots_here, channels, col_group)

    def contract(values, matrix):
        return jnp.einsum("snkcg,ngq->skcq", values, matrix, precision=exact_mode)

    real_out = contract(pieces[:, 0], cos_grid) + contract(pieces[:, 1], sin_grid)
    imag_out = contract(pieces[:, 1], cos_grid) - contract(pieces[:, 0], sin_grid)
    spectra = jnp.stack([real_out, imag_out], axis=1)
    gated_spec, filter_spec, weighted_spec = (spectra[0], spectra[1], spectra[2])
    forward_prod = product(filter_spec, gated_spec, False)
    grad_list, paired = grad_items(
        product(filter_spec, weighted_spec, True), product(gated_spec, weighted_spec, True)
    )
    spectra = jnp.stack([forward_prod] + grad_list, axis=0)
    item_count = spectra.shape[0]

    def contract(values, matrix):
        return jnp.einsum("skcq,qng->skncg", values, matrix, precision=exact_mode)

    real_out = contract(spectra[:, 0], cos_back) - contract(spectra[:, 1], sin_back)
    imag_out = contract(spectra[:, 0], sin_back) + contract(spectra[:, 1], cos_back)
    columns = jnp.stack([real_out, imag_out], axis=1).reshape(
        item_count, 2, slot_count, devices, width_cg
    )
    received = lax.all_to_all(columns, "seq", split_axis=3, concat_axis=2, tiled=True)
    item_count = received.shape[0]
    flattened = received.reshape(item_count, 2, first_len, width_cg)
    rows_real = flattened[:, 0]
    rows_imag = flattened[:, 1]
    turned_real = rows_real * cos_turn - rows_imag * sin_turn
    turned_imag = rows_imag * cos_turn + rows_real * sin_turn

    def contract(values, matrix):
        return jnp.einsum("skm,tk->stm", values, matrix, precision=exact_mode)

    real_out = contract(turned_real, cos_first) + contract(turned_imag, inv_imag)
    turned = real_out
    item_count = turned.shape[0]
    sending = turned.reshape(item_count, devices, run_count, width_cg)
    returned = lax.all_to_all(sending, "seq", split_axis=1, concat_axis=1, tiled=True)
    returned = returned.reshape(item_count, devices, run_count, channels, col_group).transpose(
        0, 3, 2, 1, 4
    )
    results = returned.reshape(item_count, channels, tokens) * out_scale
    mixed, gated_grad, filter_grad = (results[0], results[1], results[2])
    return (
        query_proj * mixed,
        out_cotangent * mixed,
        gated_grad * value_proj,
        gated_grad * key_proj,
        filter_grad,
    )


def halves(values):
    high = values.astype(jnp.bfloat16)
    return high, (values - high.astype(values.dtype)).astype(jnp.bfloat16)


def transform_tables(rows, scale):
    k1 = np.arange(rows)[:, None] * 2 + 1
    row_angle = -math.pi * ((k1 * np.arange(rows)[None, :]) % (4 * rows)) / (2 * rows)
    row_table = np.concatenate([np.cos(row_angle), np.sin(row_angle)])
    turn_period = 4 * rows * LANES
    turn_angle = -2.0 * math.pi * ((k1 * np.arange(LANES)[None, :]) % turn_period) / turn_period
    turn = np.concatenate([np.cos(turn_angle), np.sin(turn_angle)], axis=1).astype(np.float32)
    lane = np.arange(LANES)
    lane_angle = -2.0 * math.pi * ((lane[:, None] * lane[None, :]) % LANES) / LANES
    cos_lane, sin_lane = (np.cos(lane_angle), np.sin(lane_angle))
    lane_table = np.concatenate([cos_lane, sin_lane], axis=1)
    row_high, row_low = halves(row_table)
    back_high, back_low = halves(row_table.T * scale)
    lane_high, lane_low = halves(lane_table)
    return (
        np.concatenate([row_high, row_high, row_low], axis=1),
        turn,
        lane_high,
        lane_low,
        np.concatenate([back_high, back_low], axis=1),
    )


def exchange_order(devices):
    eighth = devices // 8
    return [part * eighth + i for part in (5, 2, 3, 7, 1, 4, 0, 6) for i in range(eighth)]


def pack_kernel(
    query_hbm, key_hbm, value_hbm, taps_hbm, cotangent_hbm,
    packed_ref, query_ref, key_ref, value_ref, cotangent_ref, taps_ref, arrived, *, devices, share
):
    sources = (query_hbm, key_hbm, value_hbm, taps_hbm, cotangent_hbm)
    targets = (query_ref, key_ref, value_ref, taps_ref, cotangent_ref)
    copies = [
        [
            pltpu.make_async_copy(
                source.at[pl.ds(c * devices, devices)], target.at[pl.ds(c * devices, devices)], arrived.at[c, i]
            )
            for i, (source, target) in enumerate(zip(sources, targets))
        ]
        for c in range(share)
    ]
    for group in copies:
        for copy in group:
            copy.start()
    runs = taps_ref.shape[1] // LANES
    stride = 3 * share * runs
    for c in range(share):
        for copy in copies[c]:
            copy.wait()
        for r in range(runs):
            at = (pl.ds(c * devices, devices), pl.ds(r * LANES, LANES))
            slabs = (
                key_ref[at] * value_ref[at],
                taps_ref[at],
                cotangent_ref[at] * query_ref[at],
            )
            for a, slab in enumerate(slabs):
                packed_ref[pl.ds((a * share + c) * runs + r, devices, stride=stride), :] = slab


def unpack_kernel(
    packed_ref, query_ref, key_ref, value_ref, cotangent_ref,
    out_ref, query_grad_ref, key_grad_ref, value_grad_ref, taps_grad_ref, *, devices, share
):
    runs = query_ref.shape[1] // LANES
    stride = 3 * share * runs
    for c in range(share):
        for r in range(runs):
            at = (pl.ds(c * devices, devices), pl.ds(r * LANES, LANES))
            mixed, gated_grad, taps_grad = (
                packed_ref[pl.ds((a * share + c) * runs + r, devices, stride=stride), :] for a in range(3)
            )
            out_ref[at] = query_ref[at] * mixed
            query_grad_ref[at] = cotangent_ref[at] * mixed
            key_grad_ref[at] = gated_grad * value_ref[at]
            value_grad_ref[at] = gated_grad * key_ref[at]
            taps_grad_ref[at] = taps_grad


def dot(left, right, right_dim=0):
    return lax.dot_general(
        left, right, (((1,), (right_dim,)), ((), ())), preferred_element_type=jnp.float32
    )


def channels_kernel(
    packed_ref, row_ref, turn_ref, lane_high_ref, lane_low_ref, back_ref, out_ref, *, devices, share
):
    items = 3 * share
    order = exchange_order(devices)
    runs = packed_ref.shape[0] // (devices * items)
    rows = runs * devices

    def columns(values):
        high, low = halves(values)
        return jnp.concatenate([high, low, high], axis=0)

    def along_lanes(values, high_table, low_table):
        high, low = halves(values)
        size = values.shape[0]
        both = dot(jnp.concatenate([high, low], axis=0), high_table)
        return both[:size] + both[size:] + dot(high, low_table)

    def square(table_ref, conjugate):
        cosines, sines = (table_ref[:, :LANES], table_ref[:, LANES:])
        above, below = (-sines, sines) if conjugate else (sines, -sines)
        return jnp.concatenate(
            [jnp.concatenate([cosines, above], axis=1), jnp.concatenate([below, cosines], axis=1)], axis=0
        )

    forward = (square(lane_high_ref, False), square(lane_low_ref, False))
    backward = (square(lane_high_ref, True), square(lane_low_ref, True))
    back_high, back_low = (back_ref[:, : 2 * rows], back_ref[:, 2 * rows :])
    back_table = jnp.concatenate(
        [
            jnp.concatenate([back_high, back_high], axis=1),
            jnp.concatenate([back_low, jnp.zeros_like(back_low)], axis=1),
        ],
        axis=0,
    )
    turn_real = turn_ref[:, :LANES]
    turn_imag = turn_ref[:, LANES:]
    def product(left, right):
        return jnp.concatenate(
            [left[0] * right[0] - left[1] * right[1], left[0] * right[1] + left[1] * right[0]], axis=1
        )

    def against(left, right):
        return jnp.concatenate(
            [left[0] * right[0] + left[1] * right[1], left[0] * right[1] - left[1] * right[0]], axis=1
        )

    def first_of(a):
        sequences = jnp.concatenate(
            [
                jnp.concatenate(
                    [packed_ref[pl.ds((order.index(s) * items + n) * runs, runs), :] for s in range(devices)],
                    axis=0,
                )
                for n in range(a * share, (a + 1) * share)
            ],
            axis=1,
        )
        return dot(row_ref[...], columns(sequences))

    def lines_of(first):
        turned = []
        for c in range(share):
            real = first[:rows, c * LANES : (c + 1) * LANES]
            imag = first[rows:, c * LANES : (c + 1) * LANES]
            turned.append(
                jnp.concatenate(
                    [real * turn_real - imag * turn_imag, real * turn_imag + imag * turn_real], axis=1
                )
            )
        lines = along_lanes(jnp.concatenate(turned, axis=0), *forward)
        return lines[:, :LANES], lines[:, LANES:]

    def results_of(bins):
        turned = []
        for c in range(share):
            real = bins[c * rows : (c + 1) * rows, :LANES]
            imag = bins[c * rows : (c + 1) * rows, LANES:]
            turned.append(
                jnp.concatenate(
                    [real * turn_real + imag * turn_imag, imag * turn_real - real * turn_imag], axis=0
                )
            )
        high, low = halves(jnp.concatenate(turned, axis=1))
        return dot(back_table, jnp.concatenate([high, low], axis=0))

    def store(a, both):
        results = both[:rows] + both[rows:]
        for c in range(share):
            for s in range(devices):
                out_ref[pl.ds((order.index(s) * items + a * share + c) * runs, runs), :] = results[
                    s * runs : (s + 1) * runs, c * LANES : (c + 1) * LANES
                ]

    firsts = [first_of(a) for a in range(3)]
    gated, taps, weighted = [lines_of(first) for first in firsts]
    spectra = (product(taps, gated), against(taps, weighted), against(gated, weighted))
    bins = [along_lanes(spectrum, *backward) for spectrum in spectra]
    results = [results_of(values) for values in bins]
    for a, both in enumerate(results):
        store(a, both)


def in_vmem(count):
    return [pl.BlockSpec(memory_space=pltpu.VMEM)] * count


def channels_on_devices(query_proj, key_proj, value_proj, filter_taps, out_cotangent):
    devices = lax.axis_size("seq")
    channels, tokens = filter_taps.shape
    share = channels // devices
    rows = tokens * devices // LANES
    full_len = tokens * devices
    scale = 1.0 / (full_len * math.sqrt(full_len))
    packed_shape = jax.ShapeDtypeStruct((channels * 3 * tokens // LANES, LANES), jnp.float32)
    shape = jax.ShapeDtypeStruct((channels, tokens), jnp.float32)
    sizes = {"devices": devices, "share": share}

    def call(kernel, outs, *operands, space=pltpu.VMEM, scratch=()):
        many = isinstance(outs, list)
        return pl.pallas_call(
            lambda *refs: kernel(*refs, **sizes),
            name=kernel.__name__,
            compiler_params=pltpu.CompilerParams(vmem_limit_bytes=KERNEL_VMEM),
            out_shape=outs,
            in_specs=[pl.BlockSpec(memory_space=space)] * len(operands),
            out_specs=in_vmem(len(outs)) if many else in_vmem(1)[0],
            scratch_shapes=scratch,
        )(*operands)

    def exchange(packed):
        blocks = packed.reshape(devices, -1, LANES)
        received = lax.all_to_all(
            blocks, "seq", split_axis=0, concat_axis=0, tiled=True, axis_index_groups=[exchange_order(devices)]
        )
        return received.reshape(packed.shape)

    inputs = [
        pltpu.with_memory_space_constraint(x, pltpu.HBM)
        for x in (query_proj, key_proj, value_proj, filter_taps, out_cotangent)
    ]
    packed, *gates = call(
        pack_kernel,
        [packed_shape, *[shape] * 4],
        *inputs,
        space=pltpu.HBM,
        scratch=[pltpu.VMEM((channels, tokens), jnp.float32), pltpu.SemaphoreType.DMA((share, len(inputs)))],
    )
    tables = [jnp.asarray(table) for table in transform_tables(rows, scale)]
    results = call(channels_kernel, packed_shape, exchange(packed), *tables)
    return tuple(call(unpack_kernel, [shape] * 5, exchange(results), *gates))


def per_device(query_proj, key_proj, value_proj, filter_taps, out_cotangent):
    devices = lax.axis_size("seq")
    channels, tokens = filter_taps.shape
    owns_channels = channels % devices == 0 and devices % SUBLANES == 0 and tokens % (LANES * SUBLANES) == 0
    plan = channels_on_devices if owns_channels else bins_over_devices
    return plan(query_proj, key_proj, value_proj, filter_taps, out_cotangent)


def solution(mesh):
    placed = (P("ch", "seq"), P("ch", "seq"), P("ch", "seq"), P("ch", "seq"), P("ch", "seq"))
    return jax.shard_map(
        per_device,
        mesh=mesh,
        in_specs=placed,
        out_specs=(P("ch", "seq"), P("ch", "seq"), P("ch", "seq"), P("ch", "seq"), P("ch", "seq")),
        check_vma=False,
    )
```
